512 devices in a mesh: section: 4 (over y), mp: 16 (over z), dp: 8 (over x, core).
Axes of the slice: x: 4, y: 4, z: 16, core: 2. Of those that a mesh axis runs over, the one named last changes fastest.
Arguments:
- stream: bfloat16 [16, 64, 4096], P('dp', None, 'mp'), may hold values from -6 to 6
- cotangent: bfloat16 [16, 64, 4096], P('dp', None, 'mp'), may hold values from -6 to 6
- token_ids: int32 [16, 64], P('dp'), may hold values from 0 to 32127, as said below
- buckets: int32 [64, 64], replicated, may hold values from 0 to 31, as said below
- bias_table: float32 [32, 32], P(None, 'mp'), may hold values from -300 to 300
- gain: float32 [4, 4096], P('section'), may hold values from 0.25 to 1.75
- w_query: bfloat16 [4, 4096, 2048], P('section', None, 'mp'), may hold values from -0.01171875 to 0.01171875
- w_key: bfloat16 [4, 4096, 2048], P('section', None, 'mp'), may hold values from -0.09375 to 0.09375
- w_value: bfloat16 [4, 4096, 2048], P('section', None, 'mp'), may hold values from -0.09375 to 0.09375
- w_out: bfloat16 [4, 2048, 4096], P('section', None, 'mp'), may hold values from -0.125 to 0.125
Outputs:
- input_grads: bfloat16 [4, 16, 64, 4096], P('section', 'dp', None, 'mp')
- gain_grad: float32 [4, 4096], P('section', 'mp')
- table_grad: float32 [32, 32], P(None, 'mp')
The draws below stay inside these ranges and needn't reach their ends.
Inputs may be any that keep to these rules, and one draw needn't show every extreme that they name: `token_ids`: in each sequence the ids are nonzero up to a length of 32 or more and zero after it. `buckets`: the bucket of a query and a key depends only on the key's position minus the query's: below 16 for keys at or before the query, 16 or more for keys after it.
All inputs are finite; a program needn't handle non-finite values.
Results may differ from the reference program's by a relative error of at most 0.035.
Values may be sent and summed in bfloat16 or wider, within the bound.
No kernel may reach another device: no remote copies, remote signals or barrier semaphores. Data moves between devices by JAX's collectives and lax.ppermute only.
A program may use at most 64 MiB of HBM per device.

```python
import jax
import jax.numpy as jnp
from jax import lax

D = 4096
HEADS = 32
HD = 64
BUCKETS = 32
VOCAB = 32128
SEQ = 64
LAYERS = 4
BATCH = 16
INNER = 2048
N_SECTION = 4
N_MP = 16


def draw_token_ids(key, part):
    id_key = jax.random.fold_in(key, 11)
    length_key = jax.random.fold_in(key, 12)
    drawn_ids = jax.random.randint(id_key, (BATCH, SEQ), 1, VOCAB, dtype=jnp.int32)
    lengths = jax.random.randint(length_key, (BATCH, 1), SEQ // 2, SEQ + 1, dtype=jnp.int32)
    positions = jnp.arange(SEQ, dtype=jnp.int32)[None, :]
    return jnp.where(positions < lengths, drawn_ids, 0).astype(jnp.int32)


def draw_buckets(key, part):
    exact_key = jax.random.fold_in(key, 21)
    step_key = jax.random.fold_in(key, 22)
    half_count = BUCKETS // 2
    exact_count = jax.random.randint(exact_key, (), 2, 9, dtype=jnp.int32)
    widened = jax.random.randint(step_key, (half_count - 1,), 1, 3 + SEQ // 32, dtype=jnp.int32)
    levels = jnp.arange(half_count - 1, dtype=jnp.int32)
    step_sizes = jnp.where(levels < exact_count - 1, 1, widened)
    bounds = jnp.cumsum(step_sizes)
    offsets = jnp.arange(SEQ, dtype=jnp.int32)[None, :] - jnp.arange(SEQ, dtype=jnp.int32)[:, None]
    distance = jnp.abs(offsets)
    level_index = jnp.sum((distance[:, :, None] >= bounds[None, None, :]).astype(jnp.int32), axis=2)
    return jnp.where(offsets > 0, half_count + level_index, level_index).astype(jnp.int32)


def draw_bias_table(key, part):
    table_key = jax.random.fold_in(key, 31)
    return (1.5 * jax.random.truncated_normal(table_key, -4.0, 4.0, (BUCKETS, HEADS), jnp.float32)).astype(jnp.float32)


def block_scale(key, shape, cuts, smallest, top_value):
    level, own = 1.0, jax.random.fold_in(key, 6)
    for axis_at, blocks in cuts:
        heights = jnp.exp(jax.random.uniform(jax.random.fold_in(own, axis_at), (blocks,), jnp.float32, smallest / len(cuts), top_value / len(cuts)))
        level = level * jnp.repeat(heights, shape[axis_at] // blocks).reshape([-1 if axis == axis_at else 1 for axis in range(len(shape))])
    return level


def centred(own_key, shape, scale, most, pieces=(), held_as=jnp.bfloat16):
    loudness = block_scale(own_key, shape, pieces, -0.22, 0.18) if pieces else 1.0
    array = jax.random.normal(own_key, shape, jnp.float32) * scale * loudness
    return jnp.minimum(jnp.maximum(array, -most), most).astype(held_as)


def setup_inputs(seed: int = 0) -> dict:
    arg_keys = jax.random.split(jax.random.key(seed), 11)
    return {
        "stream": centred(arg_keys[0], (BATCH, SEQ, D), 1.0, 6.0, ((0, 8), (2, 16))),
        "cotangent": centred(arg_keys[1], (BATCH, SEQ, D), 1.0, 6.0, ((0, 8), (2, 16))),
        "token_ids": draw_token_ids(jax.random.fold_in(arg_keys[10], 71), 0),
        "buckets": draw_buckets(jax.random.fold_in(arg_keys[10], 71), 0),
        "bias_table": draw_bias_table(jax.random.fold_in(arg_keys[10], 71), 0),
        "gain": jnp.clip(1.0 + 0.15 * jax.random.normal(arg_keys[5], (LAYERS, D), jnp.float32), 0.25, 1.75),
        "w_query": centred(arg_keys[6], (LAYERS, D, INNER), (D * HD) ** -0.5, 0.01171875, ((0, 4), (2, 16))),
        "w_key": centred(arg_keys[7], (LAYERS, D, INNER), D ** -0.5, 0.09375, ((0, 4), (2, 16))),
        "w_value": centred(arg_keys[8], (LAYERS, D, INNER), D ** -0.5, 0.09375, ((0, 4), (2, 16))),
        "w_out": centred(arg_keys[9], (LAYERS, INNER, D), INNER ** -0.5, 0.125, ((0, 4), (2, 16))),
    }


neg_fill = -1000000000.0
epsilon = 1e-06

def round_half(values):
    return lax.optimization_barrier(values.astype(jnp.bfloat16)).astype(jnp.float32)

def attend(proj_rows, bias_heads, mask_row):
    inner_width = HEADS * HD
    proj_f32 = proj_rows.astype(jnp.float32)
    queries = proj_f32[:, :inner_width].reshape(SEQ, HEADS, HD)
    key_rows = proj_f32[:, inner_width:2 * inner_width].reshape(SEQ, HEADS, HD)
    values = proj_f32[:, 2 * inner_width:].reshape(SEQ, HEADS, HD)
    scores = jnp.einsum('qhd,khd->hqk', queries, key_rows) + bias_heads + mask_row[None, None, :]
    row_max = lax.optimization_barrier(jnp.max(scores, axis=-1, keepdims=True))
    exp_scores = jnp.exp(scores - row_max)
    prob_full = exp_scores / lax.optimization_barrier(jnp.sum(exp_scores, axis=-1, keepdims=True))
    mixed_rows = jnp.einsum('hqk,khd->qhd', round_half(prob_full), values)
    return (mixed_rows.reshape(SEQ, inner_width).astype(jnp.bfloat16), prob_full)

def forward_layer(rows, mask_row, gain_row, w_joined, w_output, bias_heads):
    rows_f32 = rows.astype(jnp.float32)
    inv_rms = lax.rsqrt(lax.optimization_barrier(jnp.sum(rows_f32 * rows_f32, axis=1, keepdims=True)) / D + epsilon)
    scaled = (rows_f32 * gain_row[None, :]).astype(jnp.bfloat16)
    raw_proj = jnp.dot(scaled, w_joined, preferred_element_type=jnp.float32)
    proj_rows = (raw_proj * inv_rms).astype(jnp.bfloat16)
    mixed_rows, prob_full = attend(proj_rows, bias_heads, mask_row)
    branch_out = jnp.dot(mixed_rows, w_output, preferred_element_type=jnp.float32)
    next_rows = (rows_f32 + branch_out).astype(jnp.bfloat16)
    return (next_rows, (inv_rms, raw_proj, proj_rows, prob_full))

def backward_layer(upstream, rows, kept, gain_row, w_joined, w_output):
    inv_rms, raw_proj, proj_rows, prob_full = kept
    inner_width = HEADS * HD
    share_width = D // N_MP
    group_width = inner_width // N_MP
    up_blocks = upstream.astype(jnp.float32).reshape(SEQ, N_MP, share_width)
    out_blocks = w_output.astype(jnp.float32).reshape(inner_width, N_MP, share_width)
    head_parts = jnp.einsum('sjc,ijc->jsi', up_blocks, out_blocks)
    mixed_grad = lax.optimization_barrier(jnp.sum(round_half(head_parts), axis=0))
    mixed_half = round_half(mixed_grad).reshape(SEQ, HEADS, HD)
    proj_f32 = proj_rows.astype(jnp.float32)
    queries = proj_f32[:, :inner_width].reshape(SEQ, HEADS, HD)
    key_rows = proj_f32[:, inner_width:2 * inner_width].reshape(SEQ, HEADS, HD)
    values = proj_f32[:, 2 * inner_width:].reshape(SEQ, HEADS, HD)
    prob_grad = jnp.einsum('qhd,khd->hqk', mixed_half, values)
    value_grad = jnp.einsum('hqk,qhd->khd', round_half(prob_full), mixed_half)
    score_grad = prob_full * (prob_grad - lax.optimization_barrier(jnp.sum(prob_grad * prob_full, axis=-1, keepdims=True)))
    score_half = round_half(score_grad)
    query_grad = jnp.einsum('hqk,khd->qhd', score_half, key_rows)
    key_grad = jnp.einsum('hqk,qhd->khd', score_half, queries)
    proj_grad = jnp.concatenate([query_grad.reshape(SEQ, inner_width), key_grad.reshape(SEQ, inner_width), value_grad.reshape(SEQ, inner_width)], axis=1)
    radial_sum = lax.optimization_barrier(jnp.sum(proj_grad * raw_proj, axis=1, keepdims=True))
    scaled_grad = round_half(proj_grad * inv_rms).reshape(SEQ, 3, N_MP, group_width)
    joined_blocks = w_joined.astype(jnp.float32).reshape(D, 3, N_MP, group_width)
    input_parts = jnp.einsum('scjx,dcjx->jsd', scaled_grad, joined_blocks)
    normed_grad = lax.optimization_barrier(jnp.sum(round_half(input_parts), axis=0))
    rows_f32 = rows.astype(jnp.float32)
    input_grad = (upstream.astype(jnp.float32) + normed_grad * gain_row[None, :] - radial_sum * inv_rms ** 3 / D * rows_f32).astype(jnp.bfloat16)
    gain_part = lax.optimization_barrier(jnp.sum(normed_grad * rows_f32, axis=0))
    return (input_grad, gain_part, score_grad)

def reference(stream, cotangent, token_ids, buckets, bias_table, gain, w_query, w_key, w_value, w_out):
    bias_heads = jnp.transpose(bias_table[buckets], (2, 0, 1))
    key_masks = jnp.where(token_ids == 0, neg_fill, 0.0).astype(jnp.float32)
    layer_inputs = []
    layer_kept = []
    rows = stream
    for layer_index in range(N_SECTION):
        w_joined = jnp.concatenate([w_query[layer_index], w_key[layer_index], w_value[layer_index]], axis=1)

        def forward_one(pair, layer_index=layer_index, w_joined=w_joined):
            return forward_layer(pair[0], pair[1], gain[layer_index], w_joined, w_out[layer_index], bias_heads)
        next_rows, kept = lax.map(forward_one, (rows, key_masks))
        layer_inputs.append(rows)
        layer_kept.append(kept)
        rows = next_rows
    upstream = cotangent
    grads_list = [None] * N_SECTION
    gain_list = [None] * N_SECTION
    score_total = jnp.zeros((HEADS, SEQ, SEQ), jnp.float32)
    for layer_index in reversed(range(N_SECTION)):
        w_joined = jnp.concatenate([w_query[layer_index], w_key[layer_index], w_value[layer_index]], axis=1)

        def backward_one(packed, layer_index=layer_index, w_joined=w_joined):
            return backward_layer(packed[0], packed[1], packed[2], gain[layer_index], w_joined, w_out[layer_index])
        input_grad, gain_parts, score_grads = lax.map(backward_one, (upstream, layer_inputs[layer_index], layer_kept[layer_index]))
        grads_list[layer_index] = input_grad
        gain_list[layer_index] = lax.optimization_barrier(jnp.sum(gain_parts, axis=0))
        score_total = score_total + lax.optimization_barrier(jnp.sum(score_grads, axis=0))
        upstream = input_grad
    onehot = (buckets[:, :, None] == jnp.arange(BUCKETS, dtype=jnp.int32)[None, None, :]).astype(jnp.float32)
    table_grad = jnp.einsum('qkb,hqk->bh', onehot, score_total, precision=lax.Precision.HIGHEST)
    return (jnp.stack(grads_list), jnp.stack(gain_list), table_grad)
```

```python
import jax
import jax.numpy as jnp
from jax import lax
from jax.sharding import PartitionSpec as P


neg_fill = -1000000000.0
epsilon = 1e-06
f32 = jnp.float32
bf16 = jnp.bfloat16


def sent_to_all(value, axis):
    devices = lax.axis_size(axis)
    return lax.all_to_all(
        jnp.broadcast_to(value[None], (devices, *value.shape)), axis, 0, 0, tiled=True
    )


def passed_along(block, axis, distance):
    devices = range(lax.axis_size(axis))
    route = [(i - distance, i) for i in devices if i - distance in devices]
    return lax.ppermute(block, axis, route)


def side_by_side(parts):
    return jnp.concatenate([parts[i] for i in range(parts.shape[0])], axis=1)


def column_blocks(value, count):
    width = value.shape[1] // count
    return [value[:, i * width : (i + 1) * width] for i in range(count)]


def in_pieces(value):
    high = lax.reduce_precision(value, 8, 7)
    rest = value - high
    middle = lax.reduce_precision(rest, 8, 7)
    low = rest - middle
    return [high.astype(bf16), middle.astype(bf16), low.astype(bf16)]


def to_planes(pieces, planes, columns, plane_index):
    odd = plane_index % 2 == 1
    arrived = []
    for flip in (0, 1):
        route = [
            (m * columns + d, (2 * d + (m % 2 ^ flip)) * columns + m // 2)
            for m in range(planes)
            for d in range(columns)
        ]
        piece = jnp.where(odd, pieces[1 - flip], pieces[flip])
        arrived.append(lax.ppermute(piece, ("mp", "dp"), route))
    first, second = arrived
    return jnp.where(odd, second, first), jnp.where(odd, first, second)


def from_planes(halves, planes, columns, plane_index):
    odd = plane_index % 2 == 1
    arrived = []
    for flip in (0, 1):
        route = [
            (z * columns + d, (2 * d + (z % 2 ^ flip)) * columns + z // 2)
            for z in range(planes)
            for d in range(columns)
        ]
        half = jnp.where(odd, halves[1 - flip], halves[flip])
        arrived.append(lax.ppermute(half, ("mp", "dp"), route))
    first, second = arrived
    return jnp.where(odd, second, first), jnp.where(odd, first, second)


def ring_gather(part, planes, plane_index):
    whole = jnp.zeros((planes, *part.shape), part.dtype)
    zeros = (0,) * part.ndim
    whole = lax.dynamic_update_slice(whole, part[None], (plane_index, *zeros))
    ahead = [(i, (i + 1) % planes) for i in range(planes)]
    behind = [(i, (i - 1) % planes) for i in range(planes)]
    up, down = part, part
    for step in range(1, planes // 2 + 1):
        up = lax.ppermute(up, "mp", ahead)
        at = (plane_index - step) % planes
        whole = lax.dynamic_update_slice(whole, up[None], (at, *zeros))
        if step < planes // 2:
            down = lax.ppermute(down, "mp", behind)
            at = (plane_index + step) % planes
            whole = lax.dynamic_update_slice(whole, down[None], (at, *zeros))
    return whole.reshape(planes * part.shape[0], *part.shape[1:])


def per_device(
    stream, cotangent, token_ids, buckets, bias_table, gain, w_query, w_key, w_value, w_out
):
    sections = lax.axis_size("section")
    planes = lax.axis_size("mp")
    columns = lax.axis_size("dp")
    section_index = lax.axis_index("section")
    plane_index = lax.axis_index("mp")
    column_index = lax.axis_index("dp")
    bucket_count, shard_heads = bias_table.shape
    seq_len, shard_width = stream.shape[1:]
    model_width = gain.shape[1]
    width_local = 2 * shard_width
    shard_inner = w_query.shape[2]
    head_dim = shard_inner // shard_heads
    heads_local = 2 * shard_heads
    inner_width = 2 * shard_inner

    def planed(pieces):
        return to_planes(pieces, planes, columns, plane_index)

    rows = model_width // columns
    taken = [
        lax.dynamic_slice_in_dim(w[0], column_index * rows, rows) for w in (w_query, w_key, w_value)
    ]
    joined = jnp.concatenate(taken, axis=1)
    low, high = planed([joined[: rows // 2], joined[rows // 2 :]])
    at = shard_inner
    joined_part = jnp.concatenate(
        [low[:, :at], high[:, :at], low[:, at : 2 * at], high[:, at : 2 * at], low[:, 2 * at :], high[:, 2 * at :]],
        axis=1,
    )
    out_rows = w_out.shape[1] // columns
    out_taken = lax.dynamic_slice_in_dim(w_out[0], column_index * out_rows, out_rows)
    low, high = planed([out_taken[: out_rows // 2], out_taken[out_rows // 2 :]])
    out_part = jnp.concatenate([low, high], axis=1)

    stream_rows = jnp.concatenate(planed([stream[0], stream[1]]), axis=1)
    top_grad = jnp.concatenate(planed([cotangent[0], cotangent[1]]), axis=1)
    masks = jnp.where(token_ids == 0, neg_fill, 0.0).astype(f32)
    flat_bias = bias_table.reshape(1, -1)
    low, high = planed([jnp.concatenate([flat_bias, masks[i : i + 1]], axis=1) for i in (0, 1)])
    mask_row = low[0, flat_bias.shape[1] :]
    bias_local = jnp.concatenate(
        [p[0, : flat_bias.shape[1]].reshape(bucket_count, shard_heads) for p in (low, high)], axis=1
    )

    w_joined = ring_gather(joined_part, planes, plane_index)
    w_output = ring_gather(out_part, planes, plane_index)

    gain_row = gain[0]
    gain_share = lax.dynamic_slice_in_dim(gain_row, column_index * width_local, width_local)
    onehot = (
        buckets[:, :, None] == jnp.arange(bucket_count, dtype=jnp.int32)[None, None, :]
    ).astype(f32)
    bias_heads = jnp.einsum("qkb,bh->hqk", onehot, bias_local, precision=lax.Precision.HIGHEST)
    score_bias = bias_heads + mask_row[None, None, :]

    def heads_of(value):
        return value.reshape(seq_len, heads_local, head_dim)

    carried = stream_rows
    kept = None
    for tick in range(sections):
        share_rows = jnp.where(section_index == 0, stream_rows, carried) if tick else stream_rows
        full_rows = side_by_side(sent_to_all(share_rows, "dp")).astype(f32)
        scaled = (full_rows * gain_row[None, :]).astype(bf16)
        raw_proj = jnp.dot(scaled, w_joined, preferred_element_type=f32)
        square_sum = jnp.sum(full_rows * full_rows, axis=1, keepdims=True)
        inv_rms = lax.rsqrt(square_sum / model_width + epsilon)
        proj_rows = (raw_proj * inv_rms).astype(bf16)
        queries = heads_of(proj_rows[:, :inner_width])
        key_rows = heads_of(proj_rows[:, inner_width : 2 * inner_width])
        values = heads_of(proj_rows[:, 2 * inner_width :])
        scores = jnp.einsum("qhd,khd->hqk", queries, key_rows, preferred_element_type=f32)
        scores = scores + score_bias
        row_max = jnp.max(scores, axis=-1, keepdims=True)
        exp_scores = jnp.exp(scores - row_max)
        prob_full = exp_scores / jnp.sum(exp_scores, axis=-1, keepdims=True)
        mixed = jnp.einsum("hqk,khd->qhd", prob_full.astype(bf16), values, preferred_element_type=f32)
        mixed_rows = mixed.reshape(seq_len, inner_width).astype(bf16)
        now = (share_rows, inv_rms, raw_proj, proj_rows, prob_full)
        if tick == 0:
            kept = now
        else:
            mine = section_index == tick
            kept = tuple(jnp.where(mine, new, old) for new, old in zip(now, kept))
        if tick < sections - 1:
            all_mixed = side_by_side(sent_to_all(mixed_rows, "dp"))
            branch_out = jnp.dot(all_mixed, w_output, preferred_element_type=f32)
            next_share = (share_rows.astype(f32) + branch_out).astype(bf16)
            carried = passed_along(next_share, "section", 1)

    share_rows, inv_rms, raw_proj, proj_rows, prob_full = kept
    queries = heads_of(proj_rows[:, :inner_width])
    key_rows = heads_of(proj_rows[:, inner_width : 2 * inner_width])
    values = heads_of(proj_rows[:, 2 * inner_width :])
    prob_half = prob_full.astype(bf16)
    share_f32 = share_rows.astype(f32)

    grad_in = top_grad
    result = None
    for tick in range(sections):
        is_last = section_index == sections - 1
        upstream = jnp.where(is_last, top_grad, grad_in) if tick else top_grad
        out_partial = lax.dot_general(
            upstream, w_output, (((1,), (1,)), ((), ())), preferred_element_type=f32
        ).astype(bf16)
        out_parts = lax.all_to_all(
            jnp.stack(column_blocks(out_partial, columns)), "dp", 0, 0, tiled=True
        )
        mixed_grad = heads_of(jnp.sum(out_parts.astype(f32), axis=0).astype(bf16))
        prob_grad = jnp.einsum("qhd,khd->hqk", mixed_grad, values, preferred_element_type=f32)
        value_grad = jnp.einsum("hqk,qhd->khd", prob_half, mixed_grad, preferred_element_type=f32)
        score_grad = prob_full * (prob_grad - jnp.sum(prob_grad * prob_full, axis=-1, keepdims=True))
        score_half = score_grad.astype(bf16)
        query_grad = jnp.einsum("hqk,khd->qhd", score_half, key_rows, preferred_element_type=f32)
        key_grad = jnp.einsum("hqk,qhd->khd", score_half, queries, preferred_element_type=f32)
        proj_grad = jnp.concatenate(
            [g.reshape(seq_len, inner_width) for g in (query_grad, key_grad, value_grad)], axis=1
        )
        radial = jnp.sum(proj_grad * raw_proj, axis=1, keepdims=True)
        scaled_grad = (proj_grad * inv_rms).astype(bf16)
        normed_partial = lax.dot_general(
            scaled_grad, w_joined, (((1,), (1,)), ((), ())), preferred_element_type=f32
        ).astype(bf16)
        pieces = jnp.concatenate(in_pieces(radial) + [jnp.zeros((seq_len, 125), bf16)], axis=1)
        sent = jnp.stack(
            [jnp.concatenate([b, pieces], axis=1) for b in column_blocks(normed_partial, columns)]
        )
        came = jnp.sum(lax.all_to_all(sent, "dp", 0, 0, tiled=True).astype(f32), axis=0)
        normed_grad = came[:, :width_local]
        radial_sum = jnp.sum(came[:, width_local : width_local + 3], axis=1, keepdims=True)
        radial_term = radial_sum * inv_rms**3 / model_width
        input_grad = (
            upstream.astype(f32) + normed_grad * gain_share[None, :] - radial_term * share_f32
        ).astype(bf16)
        gain_part = jnp.sum(normed_grad * share_f32, axis=0, keepdims=True)
        now = (input_grad, gain_part, score_grad)
        if tick == 0:
            result = now
        else:
            mine = section_index == sections - 1 - tick
            result = tuple(jnp.where(mine, new, old) for new, old in zip(now, result))
        if tick < sections - 1:
            grad_in = passed_along(input_grad, "section", -1)

    input_grad, gain_part, score_grad = result
    table_part = jnp.einsum("qkb,hqk->hb", onehot, score_grad, precision=lax.Precision.HIGHEST)

    def halved(value):
        return column_blocks(value, 2)

    first, second = from_planes(halved(input_grad), planes, columns, plane_index)
    small = [
        jnp.concatenate([g, table_part[j * shard_heads : (j + 1) * shard_heads].reshape(1, -1)], axis=1)
        for j, g in enumerate(halved(gain_part))
    ]
    sums = from_planes(small, planes, columns, plane_index)
    everything = sent_to_all(sums[0] + sums[1], ("section", "dp")).reshape(sections, columns, -1)
    per_section = jnp.sum(everything, axis=1)
    gain_grad = lax.dynamic_index_in_dim(per_section, section_index, 0)[:, :shard_width]
    table_grad = jnp.sum(per_section[:, shard_width:], axis=0).reshape(shard_heads, bucket_count).T
    return (jnp.stack([first, second])[None], gain_grad, table_grad)


def solution(mesh):
    in_specs = (
        P("dp", None, "mp"),
        P("dp", None, "mp"),
        P("dp", None),
        P(),
        P(None, "mp"),
        P("section", None),
        P("section", None, "mp"),
        P("section", None, "mp"),
        P("section", None, "mp"),
        P("section", None, "mp"),
    )
    out_specs = (P("section", "dp", None, "mp"), P("section", "mp"), P(None, "mp"))
    return jax.shard_map(
        per_device, mesh=mesh, in_specs=in_specs, out_specs=out_specs, check_vma=False
    )
```

```python
import functools

import jax
import jax.numpy as jnp
from jax import lax
from jax.experimental import pallas as pl
from jax.experimental.pallas import tpu as pltpu
from jax.sharding import PartitionSpec as P


neg_fill = -1000000000.0
epsilon = 1e-06
f32 = jnp.float32
bf16 = jnp.bfloat16
LANES = 128
EXTRA = 16
BY_ROWS = (((1,), (1,)), ((), ()))
BY_COLUMNS = (((0,), (0,)), ((), ()))
IN_VMEM = pl.BlockSpec(memory_space=pltpu.VMEM)
IN_SMEM = pl.BlockSpec(memory_space=pltpu.SMEM)


def sent_to_all(value, axis):
    devices = lax.axis_size(axis)
    return lax.all_to_all(
        jnp.broadcast_to(value[None], (devices, *value.shape)), axis, 0, 0, tiled=True
    )


def passed_along(block, axis, distance):
    devices = range(lax.axis_size(axis))
    route = [(i - distance, i) for i in devices if i - distance in devices]
    return lax.ppermute(block, axis, route)


def plane_routes(planes, columns, back):
    return [
        [
            (m * columns + d, (2 * d + (m % 2 ^ flip)) * columns + m // 2)
            for m in range(planes)
            for d in range(columns)
        ]
        for flip in (0, 1)
    ]


def exchanged(pieces, planes, columns, plane_index):
    odd = plane_index % 2 == 1
    arrived = []
    for flip, route in enumerate(plane_routes(planes, columns, False)):
        piece = jnp.where(odd, pieces[1 - flip], pieces[flip])
        arrived.append(lax.ppermute(piece, ("mp", "dp"), route))
    first, second = arrived
    return jnp.where(odd, second, first), jnp.where(odd, first, second)


def as_rows(column):
    rows = column.shape[0]
    high = column.astype(bf16).astype(f32)
    rest = column - high
    middle = rest.astype(bf16).astype(f32)
    low = rest - middle
    lane = lax.broadcasted_iota(jnp.int32, (rows, LANES), 1)
    spread = jnp.where(lane == 0, high, jnp.where(lane == 1, middle, jnp.where(lane == 2, low, 0.0)))
    square = jnp.concatenate([spread, jnp.zeros((LANES - rows, LANES), f32)], axis=0)
    return square.T[:EXTRA].astype(bf16)


def as_column(extra, rows):
    total = jnp.sum(extra[:8], axis=0, keepdims=True)
    return jnp.broadcast_to(total, (LANES, LANES)).T[:rows]


def head_lanes(shape, which, head_dim):
    lane = lax.broadcasted_iota(jnp.int32, shape, 1)
    return (lane >= which * head_dim) & (lane < (which + 1) * head_dim)


def only_head(tile, which, head_dim):
    return jnp.where(head_lanes(tile.shape, which, head_dim), tile, jnp.zeros_like(tile))


def project_kernel(h_ref, gain_ref, w_ref, out_ref):
    seq = h_ref.shape[0]
    rows = h_ref[...].astype(f32)
    scaled = (rows * gain_ref[...]).astype(bf16)
    extra = as_rows(jnp.sum(rows * rows, axis=1, keepdims=True))
    for shard in range(w_ref.shape[0]):
        part = jnp.dot(scaled, w_ref[shard, :, : 3 * LANES], preferred_element_type=f32)
        for kind in range(3):
            at = (2 * kind + shard % 2) * seq
            out_ref[shard // 2, at : at + seq, :] = part[:, kind * LANES : (kind + 1) * LANES].astype(bf16)
    for column in range(out_ref.shape[0]):
        out_ref[column, 6 * seq :, :] = extra


def attend_kernel(tick, head_dim, model_width, last, *refs):
    if tick:
        section_ref, parts_ref, bias_ref, h_ref, w_ref, *old = refs[:10]
        refs = refs[10:]
    else:
        section_ref, parts_ref, bias_ref, h_ref, w_ref = refs[:5]
        refs = refs[5:]
    kept = refs[:5]
    h_keep, raw_keep, proj_keep, prob_keep, inv_keep = kept
    seq = h_ref.shape[0]
    total = parts_ref[0].astype(f32)
    for column in range(1, parts_ref.shape[0]):
        total = total + parts_ref[column].astype(f32)
    inv_rms = lax.rsqrt(as_column(total[6 * seq :], seq) / model_width + epsilon)
    raw = total[: 6 * seq]
    proj = (raw * jnp.concatenate([inv_rms] * 6, axis=0)).astype(bf16)
    tiles = [proj[i * seq : (i + 1) * seq] for i in range(6)]
    probs = []
    mixed = []
    for j in range(2):
        sum_tile = None
        for which in range(2):
            scores = lax.dot_general(
                only_head(tiles[j], which, head_dim), tiles[2 + j], BY_ROWS, preferred_element_type=f32
            )
            scores = scores + bias_ref[2 * j + which]
            exp_scores = jnp.exp(scores - jnp.max(scores, axis=-1, keepdims=True))
            prob = exp_scores / jnp.sum(exp_scores, axis=-1, keepdims=True)
            probs.append(prob)
            part = jnp.dot(
                prob.astype(bf16), only_head(tiles[4 + j], which, head_dim), preferred_element_type=f32
            )
            sum_tile = part if sum_tile is None else sum_tile + part
        mixed.append(sum_tile.astype(bf16))

    def store():
        h_keep[...] = h_ref[...]
        raw_keep[...] = raw
        proj_keep[...] = proj
        for i in range(4):
            prob_keep[i] = probs[i]
        inv_keep[...] = inv_rms

    if tick:
        mine = section_ref[0] == tick
        pl.when(mine)(store)

        @pl.when(jnp.logical_not(mine))
        def _():
            for new, before in zip(kept, old):
                new[...] = before[...]
    else:
        store()
    if not last:
        out_ref = refs[5]
        mixed_rows = jnp.concatenate(mixed, axis=1)
        inner = mixed_rows.shape[1]
        for shard in range(w_ref.shape[0]):
            for half in range(2):
                weights = w_ref[shard, half * inner : (half + 1) * inner, 3 * LANES :]
                at = (2 * (shard % 2) + half) * LANES
                out_ref[shard // 2, :, at : at + LANES] = jnp.dot(
                    mixed_rows, weights, preferred_element_type=f32
                ).astype(bf16)


def attend_back_kernel(tick, section, head_dim, *refs):
    if tick:
        section_ref, up_ref, raw_ref, proj_ref, prob_ref, inv_ref, w_ref, old_ref, out_ref, score_ref = refs
    else:
        section_ref, up_ref, raw_ref, proj_ref, prob_ref, inv_ref, w_ref, out_ref, score_ref = refs
    seq = up_ref.shape[1]
    inner = 2 * LANES
    grad = jnp.zeros((seq, inner), f32)
    for shard in range(w_ref.shape[0]):
        for half in range(2):
            at = (2 * (shard % 2) + half) * LANES
            grad = grad + lax.dot_general(
                up_ref[shard // 2, :, at : at + LANES],
                w_ref[shard, half * inner : (half + 1) * inner, 3 * LANES :],
                BY_ROWS,
                preferred_element_type=f32,
            )
    mixed_grad = grad.astype(bf16)
    tiles = [proj_ref[i * seq : (i + 1) * seq, :] for i in range(6)]
    grads = [None] * 6
    score_grads = []

    def add(i, value):
        grads[i] = value if grads[i] is None else grads[i] + value

    for j in range(2):
        grad_tile = mixed_grad[:, j * LANES : (j + 1) * LANES]
        for which in range(2):
            prob = prob_ref[2 * j + which]
            grad_head = only_head(grad_tile, which, head_dim)
            prob_grad = lax.dot_general(grad_head, tiles[4 + j], BY_ROWS, preferred_element_type=f32)
            add(4 + j, lax.dot_general(prob.astype(bf16), grad_head, BY_COLUMNS, preferred_element_type=f32))
            score_grad = prob * (prob_grad - jnp.sum(prob_grad * prob, axis=-1, keepdims=True))
            score_half = score_grad.astype(bf16)
            score_grads.append(score_grad)
            add(j, jnp.dot(score_half, only_head(tiles[2 + j], which, head_dim), preferred_element_type=f32))
            add(
                2 + j,
                lax.dot_general(
                    score_half, only_head(tiles[j], which, head_dim), BY_COLUMNS, preferred_element_type=f32
                ),
            )
    radial = None
    inv_rms = inv_ref[...]
    for i in range(6):
        part = grads[i] * raw_ref[i * seq : (i + 1) * seq, :]
        radial = part if radial is None else radial + part
        scaled = (grads[i] * inv_rms).astype(bf16)
        for column in range(out_ref.shape[0]):
            out_ref[column, i * seq : (i + 1) * seq, :] = scaled
    extra = as_rows(jnp.sum(radial, axis=1, keepdims=True))
    for column in range(out_ref.shape[0]):
        out_ref[column, 6 * seq :, :] = extra

    def store():
        for i in range(4):
            score_ref[i] = score_grads[i]

    if tick:
        mine = section_ref[0] == section
        pl.when(mine)(store)

        @pl.when(jnp.logical_not(mine))
        def _():
            score_ref[...] = old_ref[...]
    else:
        store()


def input_kernel(tick, section, model_width, *refs):
    if tick:
        section_ref, parts_ref, up_ref, h_ref, gain_ref, inv_ref, w_ref, old_grad, old_gain = refs[:9]
    else:
        section_ref, parts_ref, up_ref, h_ref, gain_ref, inv_ref, w_ref = refs[:7]
    grad_ref, grad_keep, gain_keep = refs[-3:]
    seq, width = up_ref.shape
    normed = jnp.zeros((seq, width), f32)
    for shard in range(w_ref.shape[0]):
        left = jnp.concatenate(
            [
                parts_ref[shard // 2, (2 * kind + shard % 2) * seq : (2 * kind + shard % 2 + 1) * seq, :]
                for kind in range(3)
            ],
            axis=1,
        )
        normed = normed + lax.dot_general(
            left, w_ref[shard, :, : 3 * LANES], BY_ROWS, preferred_element_type=f32
        )
    extra = parts_ref[0, 6 * seq :, :].astype(f32)
    for column in range(1, parts_ref.shape[0]):
        extra = extra + parts_ref[column, 6 * seq :, :].astype(f32)
    inv_rms = inv_ref[...]
    radial = as_column(extra, seq) * (inv_rms * inv_rms * inv_rms) / model_width
    rows = h_ref[...].astype(f32)
    repeats = width // LANES
    input_grad = (
        up_ref[...].astype(f32)
        + normed * gain_ref[...]
        - jnp.concatenate([radial] * repeats, axis=1) * rows
    ).astype(bf16)
    grad_ref[...] = input_grad
    gain_part = jnp.sum(normed * rows, axis=0, keepdims=True)

    def store():
        grad_keep[...] = input_grad
        gain_keep[...] = gain_part

    if tick:
        mine = section_ref[0] == section
        pl.when(mine)(store)

        @pl.when(jnp.logical_not(mine))
        def _():
            grad_keep[...] = old_grad[...]
            gain_keep[...] = old_gain[...]
    else:
        store()


def shaped(shape, dtype):
    return jax.ShapeDtypeStruct(shape, dtype)


def called(kernel, out_shape, flops, *args):
    specs = [IN_SMEM if a.dtype == jnp.int32 else IN_VMEM for a in args]
    outs = jax.tree.map(lambda _: IN_VMEM, out_shape)
    return pl.pallas_call(
        kernel,
        out_shape=out_shape,
        in_specs=specs,
        out_specs=outs,
        cost_estimate=pl.CostEstimate(flops=flops, bytes_accessed=8 << 20, transcendentals=16384),
        compiler_params=pltpu.CompilerParams(vmem_limit_bytes=40 << 20),
    )(*args)


def per_device(
    stream, cotangent, token_ids, buckets, bias_table, gain, w_query, w_key, w_value, w_out
):
    sections = lax.axis_size("section")
    planes = lax.axis_size("mp")
    columns = lax.axis_size("dp")
    section_index = lax.axis_index("section")
    plane_index = lax.axis_index("mp")
    column_index = lax.axis_index("dp")
    section_at = section_index.astype(jnp.int32).reshape(1)
    bucket_count, shard_heads = bias_table.shape
    seq_len, shard_width = stream.shape[1:]
    model_width = gain.shape[1]
    width = model_width // columns
    head_dim = w_query.shape[2] // shard_heads
    heads_local = 2 * shard_heads

    taken = [
        lax.dynamic_slice_in_dim(w[0], column_index * width, width) for w in (w_query, w_key, w_value)
    ]
    out_rows = w_out.shape[1] // columns
    out_taken = lax.dynamic_slice_in_dim(w_out[0], column_index * out_rows, out_rows)
    out_taken = jnp.concatenate([out_taken[:, :LANES], out_taken[:, LANES:]], axis=0)
    piece = jnp.concatenate([*taken, out_taken], axis=1)
    weights = lax.all_gather(piece, "mp", axis=0, tiled=True).reshape(planes, *piece.shape)

    def planed(pieces):
        return exchanged(pieces, planes, columns, plane_index)

    stream_rows = jnp.concatenate(planed([stream[0], stream[1]]), axis=1)
    top_grad = jnp.concatenate(planed([cotangent[0], cotangent[1]]), axis=1)
    masks = jnp.where(token_ids == 0, neg_fill, 0.0).astype(f32)
    flat_bias = bias_table.reshape(1, -1)
    low, high = planed([jnp.concatenate([flat_bias, masks[i : i + 1]], axis=1) for i in (0, 1)])
    mask_row = low[0, flat_bias.shape[1] :]
    bias_local = jnp.concatenate(
        [p[0, : flat_bias.shape[1]].reshape(bucket_count, shard_heads) for p in (low, high)], axis=1
    )
    gain_share = lax.dynamic_slice_in_dim(gain, column_index * width, width, axis=1)
    onehot = (
        buckets[:, :, None] == jnp.arange(bucket_count, dtype=jnp.int32)[None, None, :]
    ).astype(f32)
    bias_heads = jnp.einsum("qkb,bh->hqk", onehot, bias_local, precision=lax.Precision.HIGHEST)
    score_bias = bias_heads + mask_row[None, None, :]

    tall = 6 * seq_len
    message = shaped((columns, tall + EXTRA, LANES), bf16)
    kept_shapes = [
        shaped((seq_len, width), bf16),
        shaped((tall, LANES), f32),
        shaped((tall, LANES), bf16),
        shaped((heads_local, seq_len, seq_len), f32),
        shaped((seq_len, LANES), f32),
    ]
    project_flops = 6 * seq_len * model_width * LANES * planes
    out_flops = 2 * seq_len * 2 * LANES * model_width

    rows = stream_rows
    kept = []
    for tick in range(sections):
        last = tick == sections - 1
        sent = called(project_kernel, message, project_flops, rows, gain_share, weights)
        parts = lax.all_to_all(sent, "dp", 0, 0, tiled=True)
        outs = list(kept_shapes)
        if not last:
            outs.append(shaped((columns, seq_len, width), bf16))
        kernel = functools.partial(attend_kernel, tick, head_dim, model_width, last)
        done = called(kernel, outs, out_flops, section_at, parts, score_bias, rows, weights, *kept)
        kept = list(done[:5])
        if not last:
            branch = lax.all_to_all(done[5], "dp", 0, 0, tiled=True)
            rows = (rows.astype(f32) + jnp.sum(branch.astype(f32), axis=0)).astype(bf16)
            rows = passed_along(rows, "section", 1)
    h_rows, raw, proj, probs, inv_rms = kept

    upstream = top_grad
    scores = []
    grads = []
    for tick in range(sections):
        section = sections - 1 - tick
        up_all = sent_to_all(upstream, "dp")
        kernel = functools.partial(attend_back_kernel, tick, section, head_dim)
        outs = [message, shaped((heads_local, seq_len, seq_len), f32)]
        sent, score_grad = called(
            kernel, outs, out_flops, section_at, up_all, raw, proj, probs, inv_rms, weights, *scores
        )
        scores = [score_grad]
        parts = lax.all_to_all(sent, "dp", 0, 0, tiled=True)
        kernel = functools.partial(input_kernel, tick, section, model_width)
        outs = [
            shaped((seq_len, width), bf16),
            shaped((seq_len, width), bf16),
            shaped((1, width), f32),
        ]
        input_grad, *grads = called(
            kernel,
            outs,
            project_flops,
            section_at,
            parts,
            upstream,
            h_rows,
            gain_share,
            inv_rms,
            weights,
            *grads,
        )
        if tick < sections - 1:
            upstream = passed_along(input_grad, "section", -1)

    input_grad, gain_part = grads
    table_part = jnp.einsum("qkb,hqk->hb", onehot, scores[0], precision=lax.Precision.HIGHEST)
    half = width // 2
    small = [
        jnp.concatenate(
            [
                gain_part[:, j * half : (j + 1) * half],
                table_part[j * shard_heads : (j + 1) * shard_heads].reshape(1, -1),
            ],
            axis=1,
        )
        for j in (0, 1)
    ]
    sums = planed(small)
    first, second = planed([input_grad[:, :half], input_grad[:, half:]])
    everything = sent_to_all(sums[0] + sums[1], ("section", "dp")).reshape(sections, columns, -1)
    per_section = jnp.sum(everything, axis=1)
    gain_grad = lax.dynamic_index_in_dim(per_section, section_index, 0)[:, :shard_width]
    table_grad = jnp.sum(per_section[:, shard_width:], axis=0).reshape(shard_heads, bucket_count).T
    return (jnp.stack([first, second])[None], gain_grad, table_grad)


def solution(mesh):
    in_specs = (
        P("dp", None, "mp"),
        P("dp", None, "mp"),
        P("dp", None),
        P(),
        P(None, "mp"),
        P("section", None),
        P("section", None, "mp"),
        P("section", None, "mp"),
        P("section", None, "mp"),
        P("section", None, "mp"),
    )
    out_specs = (P("section", "dp", None, "mp"), P("section", "mp"), P(None, "mp"))
    return jax.shard_map(
        per_device, mesh=mesh, in_specs=in_specs, out_specs=out_specs, check_vma=False
    )
```

```python
import functools

import jax
import jax.numpy as jnp
from jax import lax
from jax.experimental import pallas as pl
from jax.experimental.pallas import tpu as pltpu
from jax.sharding import PartitionSpec as P


neg_fill = -1000000000.0
epsilon = 1e-06
f32 = jnp.float32
bf16 = jnp.bfloat16
LANES = 128
EXTRA = 16
BY_ROWS = (((1,), (1,)), ((), ()))
BY_COLUMNS = (((0,), (0,)), ((), ()))
IN_VMEM = pl.BlockSpec(memory_space=pltpu.VMEM)
IN_SMEM = pl.BlockSpec(memory_space=pltpu.SMEM)


def sent_to_all(value, axis):
    devices = lax.axis_size(axis)
    return lax.all_to_all(
        jnp.broadcast_to(value[None], (devices, *value.shape)), axis, 0, 0, tiled=True
    )


def passed_along(block, axis, distance):
    devices = range(lax.axis_size(axis))
    route = [(i - distance, i) for i in devices if i - distance in devices]
    return lax.ppermute(block, axis, route)


def plane_routes(planes, columns, back):
    return [
        [
            (m * columns + d, (2 * d + (m % 2 ^ flip)) * columns + m // 2)
            for m in range(planes)
            for d in range(columns)
        ]
        for flip in (0, 1)
    ]


def exchanged(pieces, planes, columns, plane_index):
    odd = plane_index % 2 == 1
    arrived = []
    for flip, route in enumerate(plane_routes(planes, columns, False)):
        piece = jnp.where(odd, pieces[1 - flip], pieces[flip])
        arrived.append(lax.ppermute(piece, ("mp", "dp"), route))
    first, second = arrived
    return jnp.where(odd, second, first), jnp.where(odd, first, second)


def as_rows(column):
    rows = column.shape[0]
    high = column.astype(bf16).astype(f32)
    rest = column - high
    middle = rest.astype(bf16).astype(f32)
    low = rest - middle
    lane = lax.broadcasted_iota(jnp.int32, (rows, LANES), 1)
    spread = jnp.where(lane == 0, high, jnp.where(lane == 1, middle, jnp.where(lane == 2, low, 0.0)))
    square = jnp.concatenate([spread, jnp.zeros((LANES - rows, LANES), f32)], axis=0)
    return square.T[:EXTRA].astype(bf16)


def three_rows(row):
    high = row.astype(bf16).astype(f32)
    rest = row - high
    middle = rest.astype(bf16).astype(f32)
    at = lax.broadcasted_iota(jnp.int32, (EXTRA, row.shape[1]), 0)
    low = rest - middle
    return jnp.where(at == 0, high, jnp.where(at == 1, middle, jnp.where(at == 2, low, 0.0)))


def in_pieces(value):
    high = lax.reduce_precision(value, 8, 7)
    rest = value - high
    middle = lax.reduce_precision(rest, 8, 7)
    return jnp.concatenate([high, middle, rest - middle], axis=0).astype(bf16)


def as_column(extra, rows):
    total = jnp.sum(extra[:8], axis=0, keepdims=True)
    return jnp.broadcast_to(total, (LANES, LANES)).T[:rows]


def head_lanes(shape, which, head_dim):
    lane = lax.broadcasted_iota(jnp.int32, shape, 1)
    return (lane >= which * head_dim) & (lane < (which + 1) * head_dim)


def only_head(tile, which, head_dim):
    return jnp.where(head_lanes(tile.shape, which, head_dim), tile, jnp.zeros_like(tile))


def project_kernel(h_ref, gain_ref, w_ref, out_ref):
    seq = h_ref.shape[0]
    rows = h_ref[...].astype(f32)
    scaled = (rows * gain_ref[...]).astype(bf16)
    extra = as_rows(jnp.sum(rows * rows, axis=1, keepdims=True))
    for shard in range(w_ref.shape[0]):
        part = jnp.dot(scaled, w_ref[shard, :, : 3 * LANES], preferred_element_type=f32)
        for kind in range(3):
            at = (2 * kind + shard % 2) * seq
            out_ref[shard // 2, at : at + seq, :] = part[:, kind * LANES : (kind + 1) * LANES].astype(bf16)
    for column in range(out_ref.shape[0]):
        out_ref[column, 6 * seq :, :] = extra


def attend_kernel(tick, head_dim, model_width, last, *refs):
    if tick:
        section_ref, parts_ref, bias_ref, h_ref, w_ref, *old = refs[:10]
        refs = refs[10:]
    else:
        section_ref, parts_ref, bias_ref, h_ref, w_ref = refs[:5]
        refs = refs[5:]
    kept = refs[:5]
    h_keep, raw_keep, proj_keep, prob_keep, inv_keep = kept
    seq = h_ref.shape[0]
    total = parts_ref[0].astype(f32)
    for column in range(1, parts_ref.shape[0]):
        total = total + parts_ref[column].astype(f32)
    inv_rms = lax.rsqrt(as_column(total[6 * seq :], seq) / model_width + epsilon)
    raw = total[: 6 * seq]
    proj = (raw * jnp.concatenate([inv_rms] * 6, axis=0)).astype(bf16)
    tiles = [proj[i * seq : (i + 1) * seq] for i in range(6)]
    probs = []
    mixed = []
    for j in range(2):
        sum_tile = None
        for which in range(2):
            scores = lax.dot_general(
                only_head(tiles[j], which, head_dim), tiles[2 + j], BY_ROWS, preferred_element_type=f32
            )
            scores = scores + bias_ref[2 * j + which]
            exp_scores = jnp.exp(scores - jnp.max(scores, axis=-1, keepdims=True))
            prob = exp_scores / jnp.sum(exp_scores, axis=-1, keepdims=True)
            probs.append(prob)
            part = jnp.dot(
                prob.astype(bf16), only_head(tiles[4 + j], which, head_dim), preferred_element_type=f32
            )
            sum_tile = part if sum_tile is None else sum_tile + part
        mixed.append(sum_tile.astype(bf16))

    def store():
        h_keep[...] = h_ref[...]
        raw_keep[...] = raw
        proj_keep[...] = proj
        for i in range(4):
            prob_keep[i] = probs[i]
        inv_keep[...] = inv_rms

    if tick:
        mine = section_ref[0] == tick
        pl.when(mine)(store)

        @pl.when(jnp.logical_not(mine))
        def _():
            for new, before in zip(kept, old):
                new[...] = before[...]
    else:
        store()
    if not last:
        out_ref = refs[5]
        mixed_rows = jnp.concatenate(mixed, axis=1)
        inner = mixed_rows.shape[1]
        for shard in range(w_ref.shape[0]):
            for half in range(2):
                weights = w_ref[shard, half * inner : (half + 1) * inner, 3 * LANES :]
                at = (2 * (shard % 2) + half) * LANES
                out_ref[shard // 2, :, at : at + LANES] = jnp.dot(
                    mixed_rows, weights, preferred_element_type=f32
                ).astype(bf16)


def attend_back_kernel(tick, section, head_dim, *refs):
    if tick:
        section_ref, up_ref, raw_ref, proj_ref, prob_ref, inv_ref, w_ref, old_ref, out_ref, score_ref = refs
    else:
        section_ref, up_ref, raw_ref, proj_ref, prob_ref, inv_ref, w_ref, out_ref, score_ref = refs
    seq = up_ref.shape[1]
    inner = 2 * LANES
    grad = jnp.zeros((seq, inner), f32)
    for shard in range(w_ref.shape[0]):
        for half in range(2):
            at = (2 * (shard % 2) + half) * LANES
            grad = grad + lax.dot_general(
                up_ref[shard // 2, :, at : at + LANES],
                w_ref[shard, half * inner : (half + 1) * inner, 3 * LANES :],
                BY_ROWS,
                preferred_element_type=f32,
            )
    mixed_grad = grad.astype(bf16)
    tiles = [proj_ref[i * seq : (i + 1) * seq, :] for i in range(6)]
    grads = [None] * 6
    score_grads = []

    def add(i, value):
        grads[i] = value if grads[i] is None else grads[i] + value

    for j in range(2):
        grad_tile = mixed_grad[:, j * LANES : (j + 1) * LANES]
        for which in range(2):
            prob = prob_ref[2 * j + which]
            grad_head = only_head(grad_tile, which, head_dim)
            prob_grad = lax.dot_general(grad_head, tiles[4 + j], BY_ROWS, preferred_element_type=f32)
            add(4 + j, lax.dot_general(prob.astype(bf16), grad_head, BY_COLUMNS, preferred_element_type=f32))
            score_grad = prob * (prob_grad - jnp.sum(prob_grad * prob, axis=-1, keepdims=True))
            score_half = score_grad.astype(bf16)
            score_grads.append(score_grad)
            add(j, jnp.dot(score_half, only_head(tiles[2 + j], which, head_dim), preferred_element_type=f32))
            add(
                2 + j,
                lax.dot_general(
                    score_half, only_head(tiles[j], which, head_dim), BY_COLUMNS, preferred_element_type=f32
                ),
            )
    radial = None
    inv_rms = inv_ref[...]
    for i in range(6):
        part = grads[i] * raw_ref[i * seq : (i + 1) * seq, :]
        radial = part if radial is None else radial + part
        scaled = (grads[i] * inv_rms).astype(bf16)
        for column in range(out_ref.shape[0]):
            out_ref[column, i * seq : (i + 1) * seq, :] = scaled
    extra = as_rows(jnp.sum(radial, axis=1, keepdims=True))
    for column in range(out_ref.shape[0]):
        out_ref[column, 6 * seq :, :] = extra

    def store():
        for i in range(4):
            score_ref[i] = score_grads[i]

    if tick:
        mine = section_ref[0] == section
        pl.when(mine)(store)

        @pl.when(jnp.logical_not(mine))
        def _():
            score_ref[...] = old_ref[...]
    else:
        store()


def input_kernel(tick, section, last, model_width, *refs):
    section_ref, parts_ref, up_ref, h_ref, gain_ref, inv_ref, w_ref, *rest = refs
    keep_ref = rest[-1]
    seq, width = up_ref.shape
    normed = jnp.zeros((seq, width), f32)
    for shard in range(w_ref.shape[0]):
        left = jnp.concatenate(
            [
                parts_ref[shard // 2, (2 * kind + shard % 2) * seq : (2 * kind + shard % 2 + 1) * seq, :]
                for kind in range(3)
            ],
            axis=1,
        )
        normed = normed + lax.dot_general(
            left, w_ref[shard, :, : 3 * LANES], BY_ROWS, preferred_element_type=f32
        )
    extra = parts_ref[0, 6 * seq :, :].astype(f32)
    for column in range(1, parts_ref.shape[0]):
        extra = extra + parts_ref[column, 6 * seq :, :].astype(f32)
    inv_rms = inv_ref[...]
    radial = as_column(extra, seq) * (inv_rms * inv_rms * inv_rms) / model_width
    rows = h_ref[...].astype(f32)
    repeats = width // LANES
    input_grad = (
        up_ref[...].astype(f32)
        + normed * gain_ref[...]
        - jnp.concatenate([radial] * repeats, axis=1) * rows
    ).astype(bf16)
    if not last:
        rest[-2][...] = input_grad
    gain_rows = three_rows(jnp.sum(normed * rows, axis=0, keepdims=True))

    def store():
        keep_ref[:seq, :] = input_grad
        keep_ref[seq:, :] = gain_rows.astype(bf16)

    if tick:
        mine = section_ref[0] == section
        pl.when(mine)(store)

        @pl.when(jnp.logical_not(mine))
        def _():
            keep_ref[...] = rest[0][...]
    else:
        store()
    if last:
        keep_ref[seq:, :] = (keep_ref[seq:, :].astype(f32) + rest[1][...].astype(f32)).astype(bf16)


def shaped(shape, dtype):
    return jax.ShapeDtypeStruct(shape, dtype)


def called(kernel, out_shape, flops, *args):
    specs = [IN_SMEM if a.dtype == jnp.int32 else IN_VMEM for a in args]
    outs = jax.tree.map(lambda _: IN_VMEM, out_shape)
    return pl.pallas_call(
        kernel,
        out_shape=out_shape,
        in_specs=specs,
        out_specs=outs,
        cost_estimate=pl.CostEstimate(flops=flops, bytes_accessed=8 << 20, transcendentals=16384),
        compiler_params=pltpu.CompilerParams(vmem_limit_bytes=16 << 20),
    )(*args)


def per_device(
    stream, cotangent, token_ids, buckets, bias_table, gain, w_query, w_key, w_value, w_out
):
    sections = lax.axis_size("section")
    planes = lax.axis_size("mp")
    columns = lax.axis_size("dp")
    section_index = lax.axis_index("section")
    plane_index = lax.axis_index("mp")
    column_index = lax.axis_index("dp")
    section_at = section_index.astype(jnp.int32).reshape(1)
    bucket_count, shard_heads = bias_table.shape
    table_size = bucket_count * shard_heads
    seq_len, shard_width = stream.shape[1:]
    model_width = gain.shape[1]
    width = model_width // columns
    head_dim = w_query.shape[2] // shard_heads
    heads_local = 2 * shard_heads

    taken = [
        lax.dynamic_slice_in_dim(w[0], column_index * width, width) for w in (w_query, w_key, w_value)
    ]
    out_rows = w_out.shape[1] // columns
    out_taken = lax.dynamic_slice_in_dim(w_out[0], column_index * out_rows, out_rows)
    out_taken = jnp.concatenate([out_taken[:, :LANES], out_taken[:, LANES:]], axis=0)
    piece = jnp.concatenate([*taken, out_taken], axis=1)
    weights = lax.all_gather(piece, "mp", axis=0, tiled=True).reshape(planes, *piece.shape)

    def planed(pieces):
        return exchanged(pieces, planes, columns, plane_index)

    stream_rows = jnp.concatenate(planed([stream[0], stream[1]]), axis=1)
    top_grad = jnp.concatenate(planed([cotangent[0], cotangent[1]]), axis=1)
    up_all = sent_to_all(top_grad, "dp")
    masks = jnp.where(token_ids == 0, neg_fill, 0.0).astype(f32)
    flat_bias = bias_table.reshape(1, -1)
    low, high = planed([jnp.concatenate([flat_bias, masks[i : i + 1]], axis=1) for i in (0, 1)])
    mask_row = low[0, flat_bias.shape[1] :]
    bias_local = jnp.concatenate(
        [p[0, : flat_bias.shape[1]].reshape(bucket_count, shard_heads) for p in (low, high)], axis=1
    )
    gain_share = lax.dynamic_slice_in_dim(gain, column_index * width, width, axis=1)
    onehot = (
        buckets[:, :, None] == jnp.arange(bucket_count, dtype=jnp.int32)[None, None, :]
    ).astype(f32)
    bias_heads = jnp.einsum("qkb,bh->hqk", onehot, bias_local, precision=lax.Precision.HIGHEST)
    score_bias = bias_heads + mask_row[None, None, :]
    stream_rows, up_all, score_bias = lax.optimization_barrier((stream_rows, up_all, score_bias))

    tall = 6 * seq_len
    message = shaped((columns, tall + EXTRA, LANES), bf16)
    kept_shapes = [
        shaped((seq_len, width), bf16),
        shaped((tall, LANES), f32),
        shaped((tall, LANES), bf16),
        shaped((heads_local, seq_len, seq_len), f32),
        shaped((seq_len, LANES), f32),
    ]
    project_flops = 6 * seq_len * model_width * LANES * planes
    out_flops = 2 * seq_len * 2 * LANES * model_width

    rows = stream_rows
    kept = []
    for tick in range(sections):
        last = tick == sections - 1
        sent = called(project_kernel, message, project_flops, rows, gain_share, weights)
        parts = lax.all_to_all(sent, "dp", 0, 0, tiled=True)
        outs = list(kept_shapes)
        if not last:
            outs.append(shaped((columns, seq_len, width), bf16))
        kernel = functools.partial(attend_kernel, tick, head_dim, model_width, last)
        done = called(kernel, outs, out_flops, section_at, parts, score_bias, rows, weights, *kept)
        kept = list(done[:5])
        if not last:
            branch = lax.all_to_all(done[5], "dp", 0, 0, tiled=True)
            rows = (rows.astype(f32) + jnp.sum(branch.astype(f32), axis=0)).astype(bf16)
            rows = passed_along(rows, "section", 1)
    h_rows, raw, proj, probs, inv_rms = kept

    upstream = top_grad
    scores = []
    grads = []
    for tick in range(sections):
        section = sections - 1 - tick
        if tick:
            up_all = sent_to_all(upstream, "dp")
        kernel = functools.partial(attend_back_kernel, tick, section, head_dim)
        outs = [message, shaped((heads_local, seq_len, seq_len), f32)]
        sent, score_grad = called(
            kernel, outs, out_flops, section_at, up_all, raw, proj, probs, inv_rms, weights, *scores
        )
        scores = [score_grad]
        last = tick == sections - 1
        if last:
            table_part = jnp.einsum("qkb,hqk->hb", onehot, score_grad, precision=lax.Precision.HIGHEST)
            table_row = jnp.pad(table_part.reshape(2, -1), ((0, 0), (0, shard_width - table_size)))
            pieces = in_pieces(table_row.reshape(1, -1))
            table_rows = jnp.pad(pieces, ((EXTRA // 2, EXTRA // 2 - 3), (0, 0)))
            sent, table_rows = lax.optimization_barrier((sent, table_rows))
            grads = [*grads, table_rows]
        parts = lax.all_to_all(sent, "dp", 0, 0, tiled=True)
        kernel = functools.partial(input_kernel, tick, section, last, model_width)
        keep = shaped((seq_len + EXTRA, width), bf16)
        outs = [keep] if last else [shaped((seq_len, width), bf16), keep]
        done = called(
            kernel,
            outs,
            project_flops,
            section_at,
            parts,
            upstream,
            h_rows,
            gain_share,
            inv_rms,
            weights,
            *grads,
        )
        grads = [done[-1]]
        if not last:
            upstream = passed_along(done[0], "section", -1)

    half = width // 2
    first, second = planed([grads[0][:, :half], grads[0][:, half:]])
    rows_in = first[seq_len:].astype(f32) + second[seq_len:].astype(f32)
    gain_in = jnp.sum(rows_in[: EXTRA // 2], axis=0, keepdims=True)
    table_in = jnp.sum(rows_in[EXTRA // 2 :, :table_size], axis=0, keepdims=True)
    sums = jnp.concatenate([gain_in, table_in], axis=1)
    everything = sent_to_all(sums, ("section", "dp")).reshape(sections, columns, -1)
    per_section = jnp.sum(everything, axis=1)
    gain_grad = lax.dynamic_index_in_dim(per_section, section_index, 0)[:, :shard_width]
    table_grad = jnp.sum(per_section[:, shard_width:], axis=0).reshape(shard_heads, bucket_count).T
    return (jnp.stack([first[:seq_len], second[:seq_len]])[None], gain_grad, table_grad)


def solution(mesh):
    in_specs = (
        P("dp", None, "mp"),
        P("dp", None, "mp"),
        P("dp", None),
        P(),
        P(None, "mp"),
        P("section", None),
        P("section", None, "mp"),
        P("section", None, "mp"),
        P("section", None, "mp"),
        P("section", None, "mp"),
    )
    out_specs = (P("section", "dp", None, "mp"), P("section", "mp"), P(None, "mp"))
    return jax.shard_map(
        per_device, mesh=mesh, in_specs=in_specs, out_specs=out_specs, check_vma=False
    )
```

```python
import functools

import jax
import jax.numpy as jnp
from jax import lax
from jax.experimental import pallas as pl
from jax.experimental.pallas import tpu as pltpu
from jax.sharding import PartitionSpec as P


neg_fill = -1000000000.0
epsilon = 1e-06
f32 = jnp.float32
bf16 = jnp.bfloat16
LANES = 128
EXTRA = 16
BY_ROWS = (((1,), (1,)), ((), ()))
BY_COLUMNS = (((0,), (0,)), ((), ()))
IN_VMEM = pl.BlockSpec(memory_space=pltpu.VMEM)
IN_SMEM = pl.BlockSpec(memory_space=pltpu.SMEM)


def sent_to_all(value, axis):
    devices = lax.axis_size(axis)
    return lax.all_to_all(
        jnp.broadcast_to(value[None], (devices, *value.shape)), axis, 0, 0, tiled=True
    )


def passed_along(block, axis, distance):
    devices = range(lax.axis_size(axis))
    route = [(i - distance, i) for i in devices if i - distance in devices]
    return lax.ppermute(block, axis, route)


def plane_routes(sections, planes, columns, taking_part):
    return [
        [
            (
                (s * planes + m) * columns + d,
                (s * planes + 2 * d + (m % 2 ^ flip)) * columns + m // 2,
            )
            for s in taking_part
            for m in range(planes)
            for d in range(columns)
        ]
        for flip in (0, 1)
    ]


def exchanged(pieces, sections, planes, columns, plane_index, taking_part):
    odd = plane_index % 2 == 1
    arrived = []
    for flip, route in enumerate(plane_routes(sections, planes, columns, taking_part)):
        piece = jnp.where(odd, pieces[1 - flip], pieces[flip])
        arrived.append(lax.ppermute(piece, ("section", "mp", "dp"), route))
    first, second = arrived
    return jnp.where(odd, second, first), jnp.where(odd, first, second)


def as_rows(column):
    rows = column.shape[0]
    high = column.astype(bf16).astype(f32)
    rest = column - high
    middle = rest.astype(bf16).astype(f32)
    low = rest - middle
    lane = lax.broadcasted_iota(jnp.int32, (rows, LANES), 1)
    spread = jnp.where(lane == 0, high, jnp.where(lane == 1, middle, jnp.where(lane == 2, low, 0.0)))
    square = jnp.concatenate([spread, jnp.zeros((LANES - rows, LANES), f32)], axis=0)
    return square.T[:EXTRA].astype(bf16)


def as_column(extra, rows):
    total = jnp.sum(extra[:8], axis=0, keepdims=True)
    return jnp.broadcast_to(total, (LANES, LANES)).T[:rows]


def head_lanes(shape, which, head_dim):
    lane = lax.broadcasted_iota(jnp.int32, shape, 1)
    return (lane >= which * head_dim) & (lane < (which + 1) * head_dim)


def only_head(tile, which, head_dim):
    return jnp.where(head_lanes(tile.shape, which, head_dim), tile, jnp.zeros_like(tile))


def cut_kernel(column_ref, query_ref, key_ref, value_ref, out_ref, piece_ref, sems):
    rows = piece_ref.shape[0]
    half = rows // 2
    column = column_ref[0]
    at = pl.ds(pl.multiple_of(column * rows, rows), rows)
    out_at = pl.ds(pl.multiple_of(column * half, half), half)
    copies = [
        pltpu.make_async_copy(
            ref.at[0, at, :], piece_ref.at[:, i * LANES : (i + 1) * LANES], sems.at[i]
        )
        for i, ref in enumerate((query_ref, key_ref, value_ref))
    ]
    for i in range(2):
        copies.append(
            pltpu.make_async_copy(
                out_ref.at[0, out_at, i * LANES : (i + 1) * LANES],
                piece_ref.at[i * half : (i + 1) * half, 3 * LANES :],
                sems.at[3 + i],
            )
        )
    for copy in copies:
        copy.start()
    for copy in copies:
        copy.wait()


def project_kernel(h_ref, gain_ref, w_ref, out_ref):
    seq = h_ref.shape[0]
    rows = h_ref[...].astype(f32)
    scaled = (rows * gain_ref[...]).astype(bf16)
    extra = as_rows(jnp.sum(rows * rows, axis=1, keepdims=True))
    for shard in range(w_ref.shape[0]):
        part = jnp.dot(scaled, w_ref[shard, :, : 3 * LANES], preferred_element_type=f32)
        for kind in range(3):
            at = (2 * kind + shard % 2) * seq
            out_ref[shard // 2, at : at + seq, :] = part[:, kind * LANES : (kind + 1) * LANES].astype(bf16)
    for column in range(out_ref.shape[0]):
        out_ref[column, 6 * seq :, :] = extra


def attend_kernel(tick, head_dim, model_width, last, *refs):
    if tick:
        section_ref, parts_ref, bias_ref, h_ref, w_ref, *old = refs[:10]
        refs = refs[10:]
    else:
        section_ref, parts_ref, bias_ref, h_ref, w_ref = refs[:5]
        refs = refs[5:]
    kept = refs[:5]
    h_keep, raw_keep, proj_keep, prob_keep, inv_keep = kept
    seq = h_ref.shape[0]
    total = parts_ref[0].astype(f32)
    for column in range(1, parts_ref.shape[0]):
        total = total + parts_ref[column].astype(f32)
    inv_rms = lax.rsqrt(as_column(total[6 * seq :], seq) / model_width + epsilon)
    raw = total[: 6 * seq]
    proj = (raw * jnp.concatenate([inv_rms] * 6, axis=0)).astype(bf16)
    tiles = [proj[i * seq : (i + 1) * seq] for i in range(6)]
    probs = []
    mixed = []
    for j in range(2):
        sum_tile = None
        for which in range(2):
            scores = lax.dot_general(
                only_head(tiles[j], which, head_dim), tiles[2 + j], BY_ROWS, preferred_element_type=f32
            )
            scores = scores + bias_ref[2 * j + which]
            exp_scores = jnp.exp(scores - jnp.max(scores, axis=-1, keepdims=True))
            prob = exp_scores / jnp.sum(exp_scores, axis=-1, keepdims=True)
            probs.append(prob)
            part = jnp.dot(
                prob.astype(bf16), only_head(tiles[4 + j], which, head_dim), preferred_element_type=f32
            )
            sum_tile = part if sum_tile is None else sum_tile + part
        mixed.append(sum_tile.astype(bf16))

    def store():
        h_keep[...] = h_ref[...]
        raw_keep[...] = raw
        proj_keep[...] = proj
        for i in range(4):
            prob_keep[i] = probs[i]
        inv_keep[...] = inv_rms

    if tick:
        mine = section_ref[0] == tick
        pl.when(mine)(store)

        @pl.when(jnp.logical_not(mine))
        def _():
            for new, before in zip(kept, old):
                new[...] = before[...]
    else:
        store()
    if not last:
        out_ref = refs[5]
        mixed_rows = jnp.concatenate(mixed, axis=1)
        inner = mixed_rows.shape[1]
        for shard in range(w_ref.shape[0]):
            for half in range(2):
                weights = w_ref[shard, half * inner : (half + 1) * inner, 3 * LANES :]
                at = (2 * (shard % 2) + half) * LANES
                out_ref[shard // 2, :, at : at + LANES] = jnp.dot(
                    mixed_rows, weights, preferred_element_type=f32
                ).astype(bf16)


def attend_back_kernel(tick, section, head_dim, *refs):
    if tick:
        section_ref, up_ref, raw_ref, proj_ref, prob_ref, inv_ref, w_ref, old_ref, out_ref, score_ref = refs
    else:
        section_ref, up_ref, raw_ref, proj_ref, prob_ref, inv_ref, w_ref, out_ref, score_ref = refs
    seq = up_ref.shape[1]
    inner = 2 * LANES
    grad = jnp.zeros((seq, inner), f32)
    for shard in range(w_ref.shape[0]):
        for half in range(2):
            at = (2 * (shard % 2) + half) * LANES
            grad = grad + lax.dot_general(
                up_ref[shard // 2, :, at : at + LANES],
                w_ref[shard, half * inner : (half + 1) * inner, 3 * LANES :],
                BY_ROWS,
                preferred_element_type=f32,
            )
    mixed_grad = grad.astype(bf16)
    tiles = [proj_ref[i * seq : (i + 1) * seq, :] for i in range(6)]
    grads = [None] * 6
    score_grads = []

    def add(i, value):
        grads[i] = value if grads[i] is None else grads[i] + value

    for j in range(2):
        grad_tile = mixed_grad[:, j * LANES : (j + 1) * LANES]
        for which in range(2):
            prob = prob_ref[2 * j + which]
            grad_head = only_head(grad_tile, which, head_dim)
            prob_grad = lax.dot_general(grad_head, tiles[4 + j], BY_ROWS, preferred_element_type=f32)
            add(4 + j, lax.dot_general(prob.astype(bf16), grad_head, BY_COLUMNS, preferred_element_type=f32))
            score_grad = prob * (prob_grad - jnp.sum(prob_grad * prob, axis=-1, keepdims=True))
            score_half = score_grad.astype(bf16)
            score_grads.append(score_grad)
            add(j, jnp.dot(score_half, only_head(tiles[2 + j], which, head_dim), preferred_element_type=f32))
            add(
                2 + j,
                lax.dot_general(
                    score_half, only_head(tiles[j], which, head_dim), BY_COLUMNS, preferred_element_type=f32
                ),
            )
    radial = None
    inv_rms = inv_ref[...]
    for i in range(6):
        part = grads[i] * raw_ref[i * seq : (i + 1) * seq, :]
        radial = part if radial is None else radial + part
        scaled = (grads[i] * inv_rms).astype(bf16)
        for column in range(out_ref.shape[0]):
            out_ref[column, i * seq : (i + 1) * seq, :] = scaled
    extra = as_rows(jnp.sum(radial, axis=1, keepdims=True))
    for column in range(out_ref.shape[0]):
        out_ref[column, 6 * seq :, :] = extra

    def store():
        for i in range(4):
            score_ref[i] = score_grads[i]

    if tick:
        mine = section_ref[0] == section
        pl.when(mine)(store)

        @pl.when(jnp.logical_not(mine))
        def _():
            score_ref[...] = old_ref[...]
    else:
        store()


def input_kernel(tick, section, last, model_width, *refs):
    section_ref, parts_ref, up_ref, h_ref, gain_ref, inv_ref, w_ref, *rest = refs
    grad_keep, gain_keep = rest[-2:]
    seq, width = up_ref.shape
    normed = jnp.zeros((seq, width), f32)
    for shard in range(w_ref.shape[0]):
        left = jnp.concatenate(
            [
                parts_ref[shard // 2, (2 * kind + shard % 2) * seq : (2 * kind + shard % 2 + 1) * seq, :]
                for kind in range(3)
            ],
            axis=1,
        )
        normed = normed + lax.dot_general(
            left, w_ref[shard, :, : 3 * LANES], BY_ROWS, preferred_element_type=f32
        )
    extra = parts_ref[0, 6 * seq :, :].astype(f32)
    for column in range(1, parts_ref.shape[0]):
        extra = extra + parts_ref[column, 6 * seq :, :].astype(f32)
    inv_rms = inv_ref[...]
    radial = as_column(extra, seq) * (inv_rms * inv_rms * inv_rms) / model_width
    rows = h_ref[...].astype(f32)
    repeats = width // LANES
    input_grad = (
        up_ref[...].astype(f32)
        + normed * gain_ref[...]
        - jnp.concatenate([radial] * repeats, axis=1) * rows
    ).astype(bf16)
    if not last:
        rest[-3][...] = input_grad
    gain_part = jnp.sum(normed * rows, axis=0, keepdims=True)

    def store():
        grad_keep[...] = input_grad
        gain_keep[...] = gain_part

    if tick:
        mine = section_ref[0] == section
        pl.when(mine)(store)

        @pl.when(jnp.logical_not(mine))
        def _():
            grad_keep[...] = rest[0][...]
            gain_keep[...] = rest[1][...]
    else:
        store()


def shaped(shape, dtype):
    return jax.ShapeDtypeStruct(shape, dtype)


def called(kernel, out_shape, flops, *args):
    specs = [IN_SMEM if a.dtype == jnp.int32 else IN_VMEM for a in args]
    outs = jax.tree.map(lambda _: IN_VMEM, out_shape)
    return pl.pallas_call(
        kernel,
        out_shape=out_shape,
        in_specs=specs,
        out_specs=outs,
        cost_estimate=pl.CostEstimate(flops=flops, bytes_accessed=8 << 20, transcendentals=16384),
        compiler_params=pltpu.CompilerParams(vmem_limit_bytes=16 << 20),
    )(*args)


def per_device(
    stream, cotangent, token_ids, buckets, bias_table, gain, w_query, w_key, w_value, w_out
):
    sections = lax.axis_size("section")
    planes = lax.axis_size("mp")
    columns = lax.axis_size("dp")
    section_index = lax.axis_index("section")
    plane_index = lax.axis_index("mp")
    column_index = lax.axis_index("dp")
    section_at = section_index.astype(jnp.int32).reshape(1)
    bucket_count, shard_heads = bias_table.shape
    seq_len, shard_width = stream.shape[1:]
    model_width = gain.shape[1]
    width = model_width // columns
    head_dim = w_query.shape[2] // shard_heads
    heads_local = 2 * shard_heads

    in_hbm = pl.BlockSpec(memory_space=pl.ANY)
    piece = pl.pallas_call(
        cut_kernel,
        out_shape=shaped((width, 4 * LANES), bf16),
        in_specs=[IN_SMEM] + [in_hbm] * 4,
        out_specs=in_hbm,
        scratch_shapes=[pltpu.SemaphoreType.DMA((5,))],
    )(column_index.astype(jnp.int32).reshape(1), w_query, w_key, w_value, w_out)
    weights = lax.all_gather(piece, "mp", axis=0, tiled=True).reshape(planes, *piece.shape)

    def planed(pieces, taking_part=range(sections)):
        return exchanged(pieces, sections, planes, columns, plane_index, taking_part)

    is_last = section_index == sections - 1
    own = [jnp.where(is_last, cotangent[i], stream[i]) for i in (0, 1)]
    entering = jnp.concatenate(planed(own, (0, sections - 1)), axis=1)
    up_all = sent_to_all(entering, "dp")
    masks = jnp.where(token_ids == 0, neg_fill, 0.0).astype(f32)
    flat_bias = bias_table.reshape(1, -1)
    low, high = planed([jnp.concatenate([flat_bias, masks[i : i + 1]], axis=1) for i in (0, 1)])
    mask_row = low[0, flat_bias.shape[1] :]
    bias_local = jnp.concatenate(
        [p[0, : flat_bias.shape[1]].reshape(bucket_count, shard_heads) for p in (low, high)], axis=1
    )
    gain_share = lax.dynamic_slice_in_dim(gain, column_index * width, width, axis=1)
    onehot = (
        buckets[:, :, None] == jnp.arange(bucket_count, dtype=jnp.int32)[None, None, :]
    ).astype(f32)
    bias_heads = jnp.einsum("qkb,bh->hqk", onehot, bias_local, precision=lax.Precision.HIGHEST)
    score_bias = bias_heads + mask_row[None, None, :]
    entering, up_all, score_bias, section_at, gain_share = lax.optimization_barrier(
        (entering, up_all, score_bias, section_at, gain_share)
    )

    tall = 6 * seq_len
    message = shaped((columns, tall + EXTRA, LANES), bf16)
    kept_shapes = [
        shaped((seq_len, width), bf16),
        shaped((tall, LANES), f32),
        shaped((tall, LANES), bf16),
        shaped((heads_local, seq_len, seq_len), f32),
        shaped((seq_len, LANES), f32),
    ]
    project_flops = 6 * seq_len * model_width * LANES * planes
    out_flops = 2 * seq_len * 2 * LANES * model_width

    rows = entering
    kept = []
    for tick in range(sections):
        last = tick == sections - 1
        sent = called(project_kernel, message, project_flops, rows, gain_share, weights)
        parts = lax.all_to_all(sent, "dp", 0, 0, tiled=True)
        outs = list(kept_shapes)
        if not last:
            outs.append(shaped((columns, seq_len, width), bf16))
        kernel = functools.partial(attend_kernel, tick, head_dim, model_width, last)
        done = called(kernel, outs, out_flops, section_at, parts, score_bias, rows, weights, *kept)
        kept = list(done[:5])
        if not last:
            branch = lax.all_to_all(done[5], "dp", 0, 0, tiled=True)
            rows = (rows.astype(f32) + jnp.sum(branch.astype(f32), axis=0)).astype(bf16)
            rows = passed_along(rows, "section", 1)
    h_rows, raw, proj, probs, inv_rms = kept

    upstream = entering
    scores = []
    grads = []
    for tick in range(sections):
        section = sections - 1 - tick
        if tick:
            up_all = sent_to_all(upstream, "dp")
        kernel = functools.partial(attend_back_kernel, tick, section, head_dim)
        outs = [message, shaped((heads_local, seq_len, seq_len), f32)]
        sent, score_grad = called(
            kernel, outs, out_flops, section_at, up_all, raw, proj, probs, inv_rms, weights, *scores
        )
        scores = [score_grad]
        last = tick == sections - 1
        parts = lax.all_to_all(sent, "dp", 0, 0, tiled=True)
        kernel = functools.partial(input_kernel, tick, section, last, model_width)
        share = shaped((seq_len, width), bf16)
        keep = [share, shaped((1, width), f32)]
        outs = keep if last else [share, *keep]
        done = called(
            kernel,
            outs,
            project_flops,
            section_at,
            parts,
            upstream,
            h_rows,
            gain_share,
            inv_rms,
            weights,
            *grads,
        )
        grads = list(done[-2:])
        if not last:
            upstream = passed_along(done[0], "section", -1)

    score_grad, gain_part = lax.optimization_barrier((scores[0], grads[1]))
    table_part = jnp.einsum("qkb,hqk->hb", onehot, score_grad, precision=lax.Precision.HIGHEST)
    half = width // 2
    small = [
        jnp.concatenate(
            [
                gain_part[:, j * half : (j + 1) * half],
                table_part[j * shard_heads : (j + 1) * shard_heads].reshape(1, -1),
            ],
            axis=1,
        )
        for j in (0, 1)
    ]
    sums = planed(small)
    sums, input_grad = lax.optimization_barrier((sums[0] + sums[1], grads[0]))
    first, second = planed([input_grad[:, :half], input_grad[:, half:]])
    everything = sent_to_all(sums, ("section", "dp")).reshape(sections, columns, -1)
    per_section = jnp.sum(everything, axis=1)
    gain_grad = lax.dynamic_index_in_dim(per_section, section_index, 0)[:, :shard_width]
    table_grad = jnp.sum(per_section[:, shard_width:], axis=0).reshape(shard_heads, bucket_count).T
    return (jnp.stack([first, second])[None], gain_grad, table_grad)


def solution(mesh):
    in_specs = (
        P("dp", None, "mp"),
        P("dp", None, "mp"),
        P("dp", None),
        P(),
        P(None, "mp"),
        P("section", None),
        P("section", None, "mp"),
        P("section", None, "mp"),
        P("section", None, "mp"),
        P("section", None, "mp"),
    )
    out_specs = (P("section", "dp", None, "mp"), P("section", "mp"), P(None, "mp"))
    return jax.shard_map(
        per_device, mesh=mesh, in_specs=in_specs, out_specs=out_specs, check_vma=False
    )
```

```python
import functools

import jax
import jax.numpy as jnp
from jax import lax
from jax.experimental import pallas as pl
from jax.experimental.pallas import tpu as pltpu
from jax.sharding import PartitionSpec as P


neg_fill = -1000000000.0
epsilon = 1e-06
f32 = jnp.float32
bf16 = jnp.bfloat16
LANES = 128
EXTRA = 16
BY_ROWS = (((1,), (1,)), ((), ()))
BY_COLUMNS = (((0,), (0,)), ((), ()))
IN_VMEM = pl.BlockSpec(memory_space=pltpu.VMEM)
IN_SMEM = pl.BlockSpec(memory_space=pltpu.SMEM)


def sent_to_all(value, axis):
    devices = lax.axis_size(axis)
    return lax.all_to_all(
        jnp.broadcast_to(value[None], (devices, *value.shape)), axis, 0, 0, tiled=True
    )


def passed_along(block, axis, distance):
    devices = range(lax.axis_size(axis))
    route = [(i - distance, i) for i in devices if i - distance in devices]
    return lax.ppermute(block, axis, route)


def plane_routes(sections, planes, columns, taking_part):
    return [
        [
            (
                (s * planes + m) * columns + d,
                (s * planes + 2 * d + (m % 2 ^ flip)) * columns + m // 2,
            )
            for s in taking_part
            for m in range(planes)
            for d in range(columns)
        ]
        for flip in (0, 1)
    ]


def exchanged(pieces, sections, planes, columns, plane_index, taking_part):
    odd = plane_index % 2 == 1
    arrived = []
    for flip, route in enumerate(plane_routes(sections, planes, columns, taking_part)):
        piece = jnp.where(odd, pieces[1 - flip], pieces[flip])
        arrived.append(lax.ppermute(piece, ("section", "mp", "dp"), route))
    first, second = arrived
    return jnp.where(odd, second, first), jnp.where(odd, first, second)


def as_rows(column):
    rows = column.shape[0]
    high = column.astype(bf16).astype(f32)
    rest = column - high
    middle = rest.astype(bf16).astype(f32)
    low = rest - middle
    lane = lax.broadcasted_iota(jnp.int32, (rows, LANES), 1)
    spread = jnp.where(lane == 0, high, jnp.where(lane == 1, middle, jnp.where(lane == 2, low, 0.0)))
    square = jnp.concatenate([spread, jnp.zeros((LANES - rows, LANES), f32)], axis=0)
    return square.T[:EXTRA].astype(bf16)


def in_pieces(row):
    high = lax.reduce_precision(row, 8, 7)
    rest = row - high
    middle = lax.reduce_precision(rest, 8, 7)
    return jnp.concatenate([high, middle, rest - middle], axis=0).astype(bf16)


def as_column(extra, rows):
    total = jnp.sum(extra[:8], axis=0, keepdims=True)
    return jnp.broadcast_to(total, (LANES, LANES)).T[:rows]


def head_lanes(shape, which, head_dim):
    lane = lax.broadcasted_iota(jnp.int32, shape, 1)
    return (lane >= which * head_dim) & (lane < (which + 1) * head_dim)


def only_head(tile, which, head_dim):
    return jnp.where(head_lanes(tile.shape, which, head_dim), tile, jnp.zeros_like(tile))


def cut_kernel(column_ref, query_ref, key_ref, value_ref, out_ref, piece_ref, sems):
    rows = piece_ref.shape[0]
    half = rows // 2
    column = column_ref[0]
    at = pl.ds(pl.multiple_of(column * rows, rows), rows)
    out_at = pl.ds(pl.multiple_of(column * half, half), half)
    copies = [
        pltpu.make_async_copy(
            ref.at[0, at, :], piece_ref.at[:, i * LANES : (i + 1) * LANES], sems.at[i]
        )
        for i, ref in enumerate((query_ref, key_ref, value_ref))
    ]
    for i in range(2):
        copies.append(
            pltpu.make_async_copy(
                out_ref.at[0, out_at, i * LANES : (i + 1) * LANES],
                piece_ref.at[i * half : (i + 1) * half, 3 * LANES :],
                sems.at[3 + i],
            )
        )
    for copy in copies:
        copy.start()
    for copy in copies:
        copy.wait()


def project_kernel(h_ref, gain_ref, w_ref, out_ref):
    seq = h_ref.shape[0]
    rows = h_ref[...].astype(f32)
    scaled = (rows * gain_ref[...]).astype(bf16)
    extra = as_rows(jnp.sum(rows * rows, axis=1, keepdims=True))
    for shard in range(w_ref.shape[0]):
        part = jnp.dot(scaled, w_ref[shard, :, : 3 * LANES], preferred_element_type=f32)
        for kind in range(3):
            at = (2 * kind + shard % 2) * seq
            out_ref[shard // 2, at : at + seq, :] = part[:, kind * LANES : (kind + 1) * LANES].astype(bf16)
    for column in range(out_ref.shape[0]):
        out_ref[column, 6 * seq :, :] = extra


def attend_kernel(tick, head_dim, model_width, last, *refs):
    if tick:
        section_ref, parts_ref, bias_ref, h_ref, w_ref, *old = refs[:10]
        refs = refs[10:]
    else:
        section_ref, parts_ref, bias_ref, h_ref, w_ref = refs[:5]
        refs = refs[5:]
    kept = refs[:5]
    h_keep, raw_keep, proj_keep, prob_keep, inv_keep = kept
    seq = h_ref.shape[0]
    total = parts_ref[0].astype(f32)
    for column in range(1, parts_ref.shape[0]):
        total = total + parts_ref[column].astype(f32)
    inv_rms = lax.rsqrt(as_column(total[6 * seq :], seq) / model_width + epsilon)
    raw = total[: 6 * seq]
    proj = (raw * jnp.concatenate([inv_rms] * 6, axis=0)).astype(bf16)
    tiles = [proj[i * seq : (i + 1) * seq] for i in range(6)]
    probs = []
    mixed = []
    for j in range(2):
        sum_tile = None
        for which in range(2):
            scores = lax.dot_general(
                only_head(tiles[j], which, head_dim), tiles[2 + j], BY_ROWS, preferred_element_type=f32
            )
            scores = scores + bias_ref[2 * j + which]
            exp_scores = jnp.exp(scores - jnp.max(scores, axis=-1, keepdims=True))
            prob = exp_scores / jnp.sum(exp_scores, axis=-1, keepdims=True)
            probs.append(prob)
            part = jnp.dot(
                prob.astype(bf16), only_head(tiles[4 + j], which, head_dim), preferred_element_type=f32
            )
            sum_tile = part if sum_tile is None else sum_tile + part
        mixed.append(sum_tile.astype(bf16))

    def store():
        h_keep[...] = h_ref[...]
        raw_keep[...] = raw
        proj_keep[...] = proj
        for i in range(4):
            prob_keep[i] = probs[i]
        inv_keep[...] = inv_rms

    if tick:
        mine = section_ref[0] == tick
        pl.when(mine)(store)

        @pl.when(jnp.logical_not(mine))
        def _():
            for new, before in zip(kept, old):
                new[...] = before[...]
    else:
        store()
    if not last:
        out_ref = refs[5]
        mixed_rows = jnp.concatenate(mixed, axis=1)
        inner = mixed_rows.shape[1]
        for shard in range(w_ref.shape[0]):
            for half in range(2):
                weights = w_ref[shard, half * inner : (half + 1) * inner, 3 * LANES :]
                at = (2 * (shard % 2) + half) * LANES
                out_ref[shard // 2, :, at : at + LANES] = jnp.dot(
                    mixed_rows, weights, preferred_element_type=f32
                ).astype(bf16)


def attend_back_kernel(tick, section, head_dim, *refs):
    if tick:
        section_ref, up_ref, raw_ref, proj_ref, prob_ref, inv_ref, w_ref, old_ref, out_ref, score_ref = refs
    else:
        section_ref, up_ref, raw_ref, proj_ref, prob_ref, inv_ref, w_ref, out_ref, score_ref = refs
    seq = up_ref.shape[1]
    inner = 2 * LANES
    grad = jnp.zeros((seq, inner), f32)
    for shard in range(w_ref.shape[0]):
        for half in range(2):
            at = (2 * (shard % 2) + half) * LANES
            grad = grad + lax.dot_general(
                up_ref[shard // 2, :, at : at + LANES],
                w_ref[shard, half * inner : (half + 1) * inner, 3 * LANES :],
                BY_ROWS,
                preferred_element_type=f32,
            )
    mixed_grad = grad.astype(bf16)
    tiles = [proj_ref[i * seq : (i + 1) * seq, :] for i in range(6)]
    grads = [None] * 6
    score_grads = []

    def add(i, value):
        grads[i] = value if grads[i] is None else grads[i] + value

    for j in range(2):
        grad_tile = mixed_grad[:, j * LANES : (j + 1) * LANES]
        for which in range(2):
            prob = prob_ref[2 * j + which]
            grad_head = only_head(grad_tile, which, head_dim)
            prob_grad = lax.dot_general(grad_head, tiles[4 + j], BY_ROWS, preferred_element_type=f32)
            add(4 + j, lax.dot_general(prob.astype(bf16), grad_head, BY_COLUMNS, preferred_element_type=f32))
            score_grad = prob * (prob_grad - jnp.sum(prob_grad * prob, axis=-1, keepdims=True))
            score_half = score_grad.astype(bf16)
            score_grads.append(score_grad)
            add(j, jnp.dot(score_half, only_head(tiles[2 + j], which, head_dim), preferred_element_type=f32))
            add(
                2 + j,
                lax.dot_general(
                    score_half, only_head(tiles[j], which, head_dim), BY_COLUMNS, preferred_element_type=f32
                ),
            )
    radial = None
    inv_rms = inv_ref[...]
    for i in range(6):
        part = grads[i] * raw_ref[i * seq : (i + 1) * seq, :]
        radial = part if radial is None else radial + part
        scaled = (grads[i] * inv_rms).astype(bf16)
        for column in range(out_ref.shape[0]):
            out_ref[column, i * seq : (i + 1) * seq, :] = scaled
    extra = as_rows(jnp.sum(radial, axis=1, keepdims=True))
    for column in range(out_ref.shape[0]):
        out_ref[column, 6 * seq :, :] = extra

    def store():
        for i in range(4):
            score_ref[i] = score_grads[i]

    if tick:
        mine = section_ref[0] == section
        pl.when(mine)(store)

        @pl.when(jnp.logical_not(mine))
        def _():
            score_ref[...] = old_ref[...]
    else:
        store()


def input_kernel(tick, section, last, model_width, *refs):
    section_ref, parts_ref, up_ref, h_ref, gain_ref, inv_ref, w_ref, *rest = refs
    grad_keep, gain_keep = rest[-2:]
    seq, width = up_ref.shape
    normed = jnp.zeros((seq, width), f32)
    for shard in range(w_ref.shape[0]):
        left = jnp.concatenate(
            [
                parts_ref[shard // 2, (2 * kind + shard % 2) * seq : (2 * kind + shard % 2 + 1) * seq, :]
                for kind in range(3)
            ],
            axis=1,
        )
        normed = normed + lax.dot_general(
            left, w_ref[shard, :, : 3 * LANES], BY_ROWS, preferred_element_type=f32
        )
    extra = parts_ref[0, 6 * seq :, :].astype(f32)
    for column in range(1, parts_ref.shape[0]):
        extra = extra + parts_ref[column, 6 * seq :, :].astype(f32)
    inv_rms = inv_ref[...]
    radial = as_column(extra, seq) * (inv_rms * inv_rms * inv_rms) / model_width
    rows = h_ref[...].astype(f32)
    repeats = width // LANES
    input_grad = (
        up_ref[...].astype(f32)
        + normed * gain_ref[...]
        - jnp.concatenate([radial] * repeats, axis=1) * rows
    ).astype(bf16)
    if not last:
        rest[-3][...] = input_grad
    gain_part = jnp.sum(normed * rows, axis=0, keepdims=True)

    def store():
        grad_keep[...] = input_grad
        gain_keep[...] = gain_part

    if tick:
        mine = section_ref[0] == section
        pl.when(mine)(store)

        @pl.when(jnp.logical_not(mine))
        def _():
            grad_keep[...] = rest[0][...]
            gain_keep[...] = rest[1][...]
    else:
        store()


def shaped(shape, dtype):
    return jax.ShapeDtypeStruct(shape, dtype)


def called(kernel, out_shape, flops, *args):
    specs = [IN_SMEM if a.dtype == jnp.int32 else IN_VMEM for a in args]
    outs = jax.tree.map(lambda _: IN_VMEM, out_shape)
    return pl.pallas_call(
        kernel,
        out_shape=out_shape,
        in_specs=specs,
        out_specs=outs,
        cost_estimate=pl.CostEstimate(flops=flops, bytes_accessed=8 << 20, transcendentals=16384),
        compiler_params=pltpu.CompilerParams(vmem_limit_bytes=16 << 20),
    )(*args)


def per_device(
    stream, cotangent, token_ids, buckets, bias_table, gain, w_query, w_key, w_value, w_out
):
    sections = lax.axis_size("section")
    planes = lax.axis_size("mp")
    columns = lax.axis_size("dp")
    section_index = lax.axis_index("section")
    plane_index = lax.axis_index("mp")
    column_index = lax.axis_index("dp")
    section_at = section_index.astype(jnp.int32).reshape(1)
    bucket_count, shard_heads = bias_table.shape
    table_size = bucket_count * shard_heads
    seq_len, shard_width = stream.shape[1:]
    model_width = gain.shape[1]
    width = model_width // columns
    head_dim = w_query.shape[2] // shard_heads
    heads_local = 2 * shard_heads

    in_hbm = pl.BlockSpec(memory_space=pl.ANY)
    piece = pl.pallas_call(
        cut_kernel,
        out_shape=shaped((width, 4 * LANES), bf16),
        in_specs=[IN_SMEM] + [in_hbm] * 4,
        out_specs=IN_VMEM,
        scratch_shapes=[pltpu.SemaphoreType.DMA((5,))],
    )(column_index.astype(jnp.int32).reshape(1), w_query, w_key, w_value, w_out)
    weights = lax.all_gather(piece, "mp", axis=0, tiled=True).reshape(planes, *piece.shape)

    def planed(pieces, taking_part=range(sections)):
        return exchanged(pieces, sections, planes, columns, plane_index, taking_part)

    is_last = section_index == sections - 1
    own = [jnp.where(is_last, cotangent[i], stream[i]) for i in (0, 1)]
    entering = jnp.concatenate(planed(own, (0, sections - 1)), axis=1)
    up_all = sent_to_all(entering, "dp")
    masks = jnp.where(token_ids == 0, neg_fill, 0.0).astype(f32)
    flat_bias = bias_table.reshape(1, -1)
    low, high = planed([jnp.concatenate([flat_bias, masks[i : i + 1]], axis=1) for i in (0, 1)])
    mask_row = low[0, flat_bias.shape[1] :]
    bias_local = jnp.concatenate(
        [p[0, : flat_bias.shape[1]].reshape(bucket_count, shard_heads) for p in (low, high)], axis=1
    )
    gain_share = lax.dynamic_slice_in_dim(gain, column_index * width, width, axis=1)
    onehot = (
        buckets[:, :, None] == jnp.arange(bucket_count, dtype=jnp.int32)[None, None, :]
    ).astype(f32)
    bias_heads = jnp.einsum("qkb,bh->hqk", onehot, bias_local, precision=lax.Precision.HIGHEST)
    score_bias = bias_heads + mask_row[None, None, :]
    entering, up_all, score_bias, section_at, gain_share = lax.optimization_barrier(
        (entering, up_all, score_bias, section_at, gain_share)
    )

    tall = 6 * seq_len
    message = shaped((columns, tall + EXTRA, LANES), bf16)
    kept_shapes = [
        shaped((seq_len, width), bf16),
        shaped((tall, LANES), f32),
        shaped((tall, LANES), bf16),
        shaped((heads_local, seq_len, seq_len), f32),
        shaped((seq_len, LANES), f32),
    ]
    project_flops = 6 * seq_len * model_width * LANES * planes
    out_flops = 2 * seq_len * 2 * LANES * model_width

    rows = entering
    kept = []
    for tick in range(sections):
        last = tick == sections - 1
        sent = called(project_kernel, message, project_flops, rows, gain_share, weights)
        parts = lax.all_to_all(sent, "dp", 0, 0, tiled=True)
        outs = list(kept_shapes)
        if not last:
            outs.append(shaped((columns, seq_len, width), bf16))
        kernel = functools.partial(attend_kernel, tick, head_dim, model_width, last)
        done = called(kernel, outs, out_flops, section_at, parts, score_bias, rows, weights, *kept)
        kept = list(done[:5])
        if not last:
            branch = lax.all_to_all(done[5], "dp", 0, 0, tiled=True)
            rows = (rows.astype(f32) + jnp.sum(branch.astype(f32), axis=0)).astype(bf16)
            rows = passed_along(rows, "section", 1)
    h_rows, raw, proj, probs, inv_rms = kept

    upstream = entering
    scores = []
    grads = []
    for tick in range(sections):
        section = sections - 1 - tick
        if tick:
            up_all = sent_to_all(upstream, "dp")
        kernel = functools.partial(attend_back_kernel, tick, section, head_dim)
        outs = [message, shaped((heads_local, seq_len, seq_len), f32)]
        sent, score_grad = called(
            kernel, outs, out_flops, section_at, up_all, raw, proj, probs, inv_rms, weights, *scores
        )
        scores = [score_grad]
        last = tick == sections - 1
        parts = lax.all_to_all(sent, "dp", 0, 0, tiled=True)
        kernel = functools.partial(input_kernel, tick, section, last, model_width)
        share = shaped((seq_len, width), bf16)
        keep = [share, shaped((1, width), f32)]
        outs = keep if last else [share, *keep]
        done = called(
            kernel,
            outs,
            project_flops,
            section_at,
            parts,
            upstream,
            h_rows,
            gain_share,
            inv_rms,
            weights,
            *grads,
        )
        grads = list(done[-2:])
        if not last:
            upstream = passed_along(done[0], "section", -1)

    score_grad, gain_part = lax.optimization_barrier((scores[0], grads[1]))
    table_part = jnp.einsum("qkb,hqk->hb", onehot, score_grad, precision=lax.Precision.HIGHEST)
    table_row = jnp.pad(table_part.reshape(2, -1), ((0, 0), (0, shard_width - table_size)))
    riding = jnp.concatenate(
        [
            in_pieces(gain_part),
            in_pieces(table_row.reshape(1, -1)),
            jnp.zeros((EXTRA - 6, width), bf16),
        ],
        axis=0,
    )
    going = jnp.concatenate([grads[0], riding], axis=0)
    first, second = planed([going[:, :shard_width], going[:, shard_width:]])
    rows_in = first[seq_len:].astype(f32) + second[seq_len:].astype(f32)
    gain_in = jnp.sum(rows_in[:3], axis=0, keepdims=True)
    table_in = jnp.sum(rows_in[3:6, :table_size], axis=0, keepdims=True)
    sums = jnp.concatenate([gain_in, table_in], axis=1)
    everything = sent_to_all(sums, ("section", "dp")).reshape(sections, columns, -1)
    per_section = jnp.sum(everything, axis=1)
    gain_grad = lax.dynamic_index_in_dim(per_section, section_index, 0)[:, :shard_width]
    table_grad = jnp.sum(per_section[:, shard_width:], axis=0).reshape(shard_heads, bucket_count).T
    return (jnp.stack([first[:seq_len], second[:seq_len]])[None], gain_grad, table_grad)


def solution(mesh):
    in_specs = (
        P("dp", None, "mp"),
        P("dp", None, "mp"),
        P("dp", None),
        P(),
        P(None, "mp"),
        P("section", None),
        P("section", None, "mp"),
        P("section", None, "mp"),
        P("section", None, "mp"),
        P("section", None, "mp"),
    )
    out_specs = (P("section", "dp", None, "mp"), P("section", "mp"), P(None, "mp"))
    return jax.shard_map(
        per_device, mesh=mesh, in_specs=in_specs, out_specs=out_specs, check_vma=False
    )
```

```python
import functools

import jax
import jax.numpy as jnp
from jax import lax
from jax.experimental import pallas as pl
from jax.experimental.pallas import tpu as pltpu
from jax.sharding import PartitionSpec as P


neg_fill = -1000000000.0
epsilon = 1e-06
f32 = jnp.float32
bf16 = jnp.bfloat16
LANES = 128
EXTRA = 16
BY_ROWS = (((1,), (1,)), ((), ()))
BY_COLUMNS = (((0,), (0,)), ((), ()))
IN_VMEM = pl.BlockSpec(memory_space=pltpu.VMEM)
IN_SMEM = pl.BlockSpec(memory_space=pltpu.SMEM)


def sent_to_all(value, axis):
    devices = lax.axis_size(axis)
    return lax.all_to_all(
        jnp.broadcast_to(value[None], (devices, *value.shape)), axis, 0, 0, tiled=True
    )


def passed_along(block, axis, distance):
    devices = range(lax.axis_size(axis))
    route = [(i - distance, i) for i in devices if i - distance in devices]
    return lax.ppermute(block, axis, route)


def spread(index, planes):
    side = 4
    return (index % side) * (planes // side) + index // side


def plane_routes(sections, planes, columns, taking_part, back):
    routes = []
    for flip in (0, 1):
        route = []
        for s in taking_part:
            for m in range(planes):
                for d in range(columns):
                    sequence = 2 * d + (m % 2 ^ flip)
                    home = (s * planes + m) * columns + d
                    work = (s * planes + spread(sequence, planes)) * columns + m // 2
                    route.append((work, home) if back else (home, work))
        routes.append(route)
    return routes


def exchanged(pieces, sections, planes, columns, plane_index, taking_part, back=False):
    home_odd = plane_index % 2 == 1
    work_odd = spread(plane_index, planes) % 2 == 1
    sent_odd, came_odd = (work_odd, home_odd) if back else (home_odd, work_odd)
    arrived = []
    for flip, route in enumerate(plane_routes(sections, planes, columns, taking_part, back)):
        piece = jnp.where(sent_odd, pieces[1 - flip], pieces[flip])
        arrived.append(lax.ppermute(piece, ("section", "mp", "dp"), route))
    first, second = arrived
    return jnp.where(came_odd, second, first), jnp.where(came_odd, first, second)


def as_rows(column):
    rows = column.shape[0]
    high = column.astype(bf16).astype(f32)
    rest = column - high
    middle = rest.astype(bf16).astype(f32)
    low = rest - middle
    lane = lax.broadcasted_iota(jnp.int32, (rows, LANES), 1)
    spread = jnp.where(lane == 0, high, jnp.where(lane == 1, middle, jnp.where(lane == 2, low, 0.0)))
    square = jnp.concatenate([spread, jnp.zeros((LANES - rows, LANES), f32)], axis=0)
    return square.T[:EXTRA].astype(bf16)


def in_pieces(row):
    high = lax.reduce_precision(row, 8, 7)
    rest = row - high
    middle = lax.reduce_precision(rest, 8, 7)
    return jnp.concatenate([high, middle, rest - middle], axis=0).astype(bf16)


def as_column(extra, rows):
    total = jnp.sum(extra[:8], axis=0, keepdims=True)
    return jnp.broadcast_to(total, (LANES, LANES)).T[:rows]


def head_lanes(shape, which, head_dim):
    lane = lax.broadcasted_iota(jnp.int32, shape, 1)
    return (lane >= which * head_dim) & (lane < (which + 1) * head_dim)


def only_head(tile, which, head_dim):
    return jnp.where(head_lanes(tile.shape, which, head_dim), tile, jnp.zeros_like(tile))


def cut_kernel(column_ref, query_ref, key_ref, value_ref, out_ref, piece_ref, block_ref, sems):
    rows = piece_ref.shape[0]
    out_rows = block_ref.shape[0]
    column = column_ref[0]
    at = pl.ds(pl.multiple_of(column * rows, rows), rows)
    out_at = pl.ds(pl.multiple_of(column * out_rows, out_rows), out_rows)
    copies = [
        pltpu.make_async_copy(
            ref.at[0, at, :], piece_ref.at[:, i * LANES : (i + 1) * LANES], sems.at[i]
        )
        for i, ref in enumerate((query_ref, key_ref, value_ref))
    ]
    copies.append(pltpu.make_async_copy(out_ref.at[0, out_at, :], block_ref, sems.at[3]))
    for copy in copies:
        copy.start()
    for copy in copies:
        copy.wait()


def order_kernel(plane_ref, *refs):
    *blocks, out_ref = refs
    planes = len(blocks)
    for k, block in enumerate(blocks):
        out_ref[lax.rem(plane_ref[0] + planes - k, planes)] = block[...]


def project_kernel(h_ref, gain_ref, w_ref, out_ref):
    seq = h_ref.shape[0]
    rows = h_ref[...].astype(f32)
    scaled = (rows * gain_ref[...]).astype(bf16)
    extra = as_rows(jnp.sum(rows * rows, axis=1, keepdims=True))
    for shard in range(w_ref.shape[0]):
        part = jnp.dot(scaled, w_ref[shard], preferred_element_type=f32)
        for kind in range(3):
            at = (2 * kind + shard % 2) * seq
            out_ref[shard // 2, at : at + seq, :] = part[:, kind * LANES : (kind + 1) * LANES].astype(bf16)
    for column in range(out_ref.shape[0]):
        out_ref[column, 6 * seq :, :] = extra


def attend_kernel(tick, head_dim, model_width, last_section, *refs):
    last = tick == last_section
    if tick:
        section_ref, parts_ref, bias_ref, h_ref, w_ref, *old = refs[:10]
        refs = refs[10:]
    else:
        section_ref, parts_ref, bias_ref, h_ref, w_ref = refs[:5]
        refs = refs[5:]
    kept = refs[:5]
    h_keep, raw_keep, proj_keep, prob_keep, inv_keep = kept
    seq = h_ref.shape[0]
    total = parts_ref[0].astype(f32)
    for column in range(1, parts_ref.shape[0]):
        total = total + parts_ref[column].astype(f32)
    inv_rms = lax.rsqrt(as_column(total[6 * seq :], seq) / model_width + epsilon)
    raw = total[: 6 * seq]
    proj = (raw * jnp.concatenate([inv_rms] * 6, axis=0)).astype(bf16)
    tiles = [proj[i * seq : (i + 1) * seq] for i in range(6)]
    probs = []
    mixed = []
    for j in range(2):
        sum_tile = None
        for which in range(2):
            scores = lax.dot_general(
                only_head(tiles[j], which, head_dim), tiles[2 + j], BY_ROWS, preferred_element_type=f32
            )
            scores = scores + bias_ref[2 * j + which]
            exp_scores = jnp.exp(scores - jnp.max(scores, axis=-1, keepdims=True))
            prob = exp_scores / jnp.sum(exp_scores, axis=-1, keepdims=True)
            probs.append(prob)
            part = jnp.dot(
                prob.astype(bf16), only_head(tiles[4 + j], which, head_dim), preferred_element_type=f32
            )
            sum_tile = part if sum_tile is None else sum_tile + part
        mixed.append(sum_tile.astype(bf16))

    def store():
        h_keep[...] = h_ref[...]
        raw_keep[...] = raw
        proj_keep[...] = proj
        for i in range(4):
            prob_keep[i] = probs[i]
        inv_keep[...] = inv_rms

    if tick:
        mine = section_ref[0] == tick
        pl.when(mine)(store)

        @pl.when(jnp.logical_not(mine))
        def _():
            for new, before in zip(kept, old):
                new[...] = before[...]
    else:
        store()
    if not last:
        out_ref = refs[5]
        mixed_rows = jnp.concatenate(mixed, axis=1)

        def send():
            inner = mixed_rows.shape[1]
            for shard in range(w_ref.shape[0]):
                for half in range(2):
                    weights = w_ref[shard, :, half * LANES : (half + 1) * LANES]
                    at = (2 * (shard % 2) + half) * LANES
                    out_ref[shard // 2, :, at : at + LANES] = jnp.dot(
                        mixed_rows, weights, preferred_element_type=f32
                    ).astype(bf16)

        if tick:
            send()
        else:
            pl.when(section_ref[0] != last_section)(send)

            @pl.when(section_ref[0] == last_section)
            def _():
                for column in range(out_ref.shape[0]):
                    out_ref[column] = h_ref[...]


def attend_back_kernel(tick, section, head_dim, *refs):
    if tick:
        section_ref, up_ref, raw_ref, proj_ref, prob_ref, inv_ref, w_ref, old_ref, out_ref, score_ref = refs
    else:
        section_ref, up_ref, raw_ref, proj_ref, prob_ref, inv_ref, w_ref, out_ref, score_ref = refs
    seq = up_ref.shape[1]
    inner = 2 * LANES
    grad = jnp.zeros((seq, inner), f32)
    for shard in range(w_ref.shape[0]):
        for half in range(2):
            at = (2 * (shard % 2) + half) * LANES
            grad = grad + lax.dot_general(
                up_ref[shard // 2, :, at : at + LANES],
                w_ref[shard, :, half * LANES : (half + 1) * LANES],
                BY_ROWS,
                preferred_element_type=f32,
            )
    mixed_grad = grad.astype(bf16)
    tiles = [proj_ref[i * seq : (i + 1) * seq, :] for i in range(6)]
    grads = [None] * 6
    score_grads = []

    def add(i, value):
        grads[i] = value if grads[i] is None else grads[i] + value

    for j in range(2):
        grad_tile = mixed_grad[:, j * LANES : (j + 1) * LANES]
        for which in range(2):
            prob = prob_ref[2 * j + which]
            grad_head = only_head(grad_tile, which, head_dim)
            prob_grad = lax.dot_general(grad_head, tiles[4 + j], BY_ROWS, preferred_element_type=f32)
            add(4 + j, lax.dot_general(prob.astype(bf16), grad_head, BY_COLUMNS, preferred_element_type=f32))
            score_grad = prob * (prob_grad - jnp.sum(prob_grad * prob, axis=-1, keepdims=True))
            score_half = score_grad.astype(bf16)
            score_grads.append(score_grad)
            add(j, jnp.dot(score_half, only_head(tiles[2 + j], which, head_dim), preferred_element_type=f32))
            add(
                2 + j,
                lax.dot_general(
                    score_half, only_head(tiles[j], which, head_dim), BY_COLUMNS, preferred_element_type=f32
                ),
            )
    radial = None
    inv_rms = inv_ref[...]
    for i in range(6):
        part = grads[i] * raw_ref[i * seq : (i + 1) * seq, :]
        radial = part if radial is None else radial + part
        scaled = (grads[i] * inv_rms).astype(bf16)
        for column in range(out_ref.shape[0]):
            out_ref[column, i * seq : (i + 1) * seq, :] = scaled
    extra = as_rows(jnp.sum(radial, axis=1, keepdims=True))
    for column in range(out_ref.shape[0]):
        out_ref[column, 6 * seq :, :] = extra

    def store():
        for i in range(4):
            score_ref[i] = score_grads[i]

    if tick:
        mine = section_ref[0] == section
        pl.when(mine)(store)

        @pl.when(jnp.logical_not(mine))
        def _():
            score_ref[...] = old_ref[...]
    else:
        store()


def input_kernel(tick, section, last, model_width, *refs):
    section_ref, parts_ref, up_ref, h_ref, gain_ref, inv_ref, w_ref, *rest = refs
    grad_keep, gain_keep = rest[-2:]
    seq, width = up_ref.shape
    normed = jnp.zeros((seq, width), f32)
    for shard in range(w_ref.shape[0]):
        left = jnp.concatenate(
            [
                parts_ref[shard // 2, (2 * kind + shard % 2) * seq : (2 * kind + shard % 2 + 1) * seq, :]
                for kind in range(3)
            ],
            axis=1,
        )
        normed = normed + lax.dot_general(
            left, w_ref[shard], BY_ROWS, preferred_element_type=f32
        )
    extra = parts_ref[0, 6 * seq :, :].astype(f32)
    for column in range(1, parts_ref.shape[0]):
        extra = extra + parts_ref[column, 6 * seq :, :].astype(f32)
    inv_rms = inv_ref[...]
    radial = as_column(extra, seq) * (inv_rms * inv_rms * inv_rms) / model_width
    rows = h_ref[...].astype(f32)
    repeats = width // LANES
    input_grad = (
        up_ref[...].astype(f32)
        + normed * gain_ref[...]
        - jnp.concatenate([radial] * repeats, axis=1) * rows
    ).astype(bf16)
    if not last:
        rest[-3][...] = input_grad
    gain_part = jnp.sum(normed * rows, axis=0, keepdims=True)

    def store():
        grad_keep[...] = input_grad
        gain_keep[...] = gain_part

    if tick:
        mine = section_ref[0] == section
        pl.when(mine)(store)

        @pl.when(jnp.logical_not(mine))
        def _():
            grad_keep[...] = rest[0][...]
            gain_keep[...] = rest[1][...]
    else:
        store()


def shaped(shape, dtype):
    return jax.ShapeDtypeStruct(shape, dtype)


def called(kernel, out_shape, flops, *args):
    specs = [IN_SMEM if a.dtype == jnp.int32 else IN_VMEM for a in args]
    outs = jax.tree.map(lambda _: IN_VMEM, out_shape)
    return pl.pallas_call(
        kernel,
        out_shape=out_shape,
        in_specs=specs,
        out_specs=outs,
        cost_estimate=pl.CostEstimate(flops=flops, bytes_accessed=8 << 20, transcendentals=16384),
        compiler_params=pltpu.CompilerParams(vmem_limit_bytes=16 << 20),
    )(*args)


def per_device(
    stream, cotangent, token_ids, buckets, bias_table, gain, w_query, w_key, w_value, w_out
):
    sections = lax.axis_size("section")
    planes = lax.axis_size("mp")
    columns = lax.axis_size("dp")
    section_index = lax.axis_index("section")
    plane_index = lax.axis_index("mp")
    column_index = lax.axis_index("dp")
    section_at = section_index.astype(jnp.int32).reshape(1)
    bucket_count, shard_heads = bias_table.shape
    table_size = bucket_count * shard_heads
    seq_len, shard_width = stream.shape[1:]
    model_width = gain.shape[1]
    width = model_width // columns
    head_dim = w_query.shape[2] // shard_heads
    heads_local = 2 * shard_heads

    in_hbm = pl.BlockSpec(memory_space=pl.ANY)
    out_rows = w_out.shape[1] // columns
    piece, block = pl.pallas_call(
        cut_kernel,
        out_shape=[shaped((width, 3 * LANES), bf16), shaped((out_rows, shard_width), bf16)],
        in_specs=[IN_SMEM] + [in_hbm] * 4,
        out_specs=[IN_VMEM, IN_VMEM],
        scratch_shapes=[pltpu.SemaphoreType.DMA((4,))],
    )(column_index.astype(jnp.int32).reshape(1), w_query, w_key, w_value, w_out)
    weights = lax.all_gather(piece, "mp", axis=0, tiled=True).reshape(planes, *piece.shape)
    up, down = [block], [block]
    for _ in range(planes // 2):
        up.append(lax.ppermute(up[-1], "mp", [(i, (i + 1) % planes) for i in range(planes)]))
    for _ in range(planes // 2 - 1):
        down.append(lax.ppermute(down[-1], "mp", [(i, (i - 1) % planes) for i in range(planes)]))
    plane_at = plane_index.astype(jnp.int32).reshape(1)
    out_weights = called(
        order_kernel, shaped((planes, *block.shape), bf16), 1, plane_at, *up, *down[:0:-1]
    )

    def planed(pieces, taking_part=range(sections), back=False):
        return exchanged(pieces, sections, planes, columns, plane_index, taking_part, back)

    is_last = section_index == sections - 1
    own = [jnp.where(is_last, cotangent[i], stream[i]) for i in (0, 1)]
    entering = jnp.concatenate(planed(own, (0, sections - 1)), axis=1)
    masks = jnp.where(token_ids == 0, neg_fill, 0.0).astype(f32)
    flat_bias = bias_table.reshape(1, -1)
    low, high = planed([jnp.concatenate([flat_bias, masks[i : i + 1]], axis=1) for i in (0, 1)])
    mask_row = low[0, flat_bias.shape[1] :]
    bias_local = jnp.concatenate(
        [p[0, : flat_bias.shape[1]].reshape(bucket_count, shard_heads) for p in (low, high)], axis=1
    )
    gain_share = lax.dynamic_slice_in_dim(gain, column_index * width, width, axis=1)
    onehot = (
        buckets[:, :, None] == jnp.arange(bucket_count, dtype=jnp.int32)[None, None, :]
    ).astype(f32)
    bias_heads = jnp.einsum("qkb,bh->hqk", onehot, bias_local, precision=lax.Precision.HIGHEST)
    score_bias = bias_heads + mask_row[None, None, :]
    entering, score_bias, section_at, gain_share, out_weights = lax.optimization_barrier(
        (entering, score_bias, section_at, gain_share, out_weights)
    )

    tall = 6 * seq_len
    message = shaped((columns, tall + EXTRA, LANES), bf16)
    kept_shapes = [
        shaped((seq_len, width), bf16),
        shaped((tall, LANES), f32),
        shaped((tall, LANES), bf16),
        shaped((heads_local, seq_len, seq_len), f32),
        shaped((seq_len, LANES), f32),
    ]
    project_flops = 6 * seq_len * model_width * LANES * planes
    out_flops = 2 * seq_len * 2 * LANES * model_width

    rows = entering
    kept = []
    for tick in range(sections):
        last = tick == sections - 1
        sent = called(project_kernel, message, project_flops, rows, gain_share, weights)
        parts = lax.all_to_all(sent, "dp", 0, 0, tiled=True)
        outs = list(kept_shapes)
        if not last:
            outs.append(shaped((columns, seq_len, width), bf16))
        kernel = functools.partial(attend_kernel, tick, head_dim, model_width, sections - 1)
        done = called(kernel, outs, out_flops, section_at, parts, score_bias, rows, out_weights, *kept)
        kept = list(done[:5])
        if not last:
            branch = lax.all_to_all(done[5], "dp", 0, 0, tiled=True)
            if tick == 0:
                up_all = branch
            rows = (rows.astype(f32) + jnp.sum(branch.astype(f32), axis=0)).astype(bf16)
            rows = passed_along(rows, "section", 1)
    h_rows, raw, proj, probs, inv_rms = kept

    upstream = entering
    scores = []
    grads = []
    for tick in range(sections):
        section = sections - 1 - tick
        if tick:
            up_all = sent_to_all(upstream, "dp")
        kernel = functools.partial(attend_back_kernel, tick, section, head_dim)
        outs = [message, shaped((heads_local, seq_len, seq_len), f32)]
        sent, score_grad = called(
            kernel, outs, out_flops, section_at, up_all, raw, proj, probs, inv_rms, out_weights, *scores
        )
        scores = [score_grad]
        last = tick == sections - 1
        parts = lax.all_to_all(sent, "dp", 0, 0, tiled=True)
        kernel = functools.partial(input_kernel, tick, section, last, model_width)
        share = shaped((seq_len, width), bf16)
        keep = [share, shaped((1, width), f32)]
        outs = keep if last else [share, *keep]
        done = called(
            kernel,
            outs,
            project_flops,
            section_at,
            parts,
            upstream,
            h_rows,
            gain_share,
            inv_rms,
            weights,
            *grads,
        )
        grads = list(done[-2:])
        if not last:
            upstream = passed_along(done[0], "section", -1)

    score_grad, gain_part = lax.optimization_barrier((scores[0], grads[1]))
    table_part = jnp.einsum("qkb,hqk->hb", onehot, score_grad, precision=lax.Precision.HIGHEST)
    table_row = jnp.pad(table_part.reshape(2, -1), ((0, 0), (0, shard_width - table_size)))
    riding = jnp.concatenate(
        [
            in_pieces(gain_part),
            in_pieces(table_row.reshape(1, -1)),
            jnp.zeros((EXTRA - 6, width), bf16),
        ],
        axis=0,
    )
    going = jnp.concatenate([grads[0], riding], axis=0)
    first, second = planed([going[:, :shard_width], going[:, shard_width:]], back=True)
    rows_in = first[seq_len:].astype(f32) + second[seq_len:].astype(f32)
    gain_in = jnp.sum(rows_in[:3], axis=0, keepdims=True)
    table_in = jnp.sum(rows_in[3:6, :table_size], axis=0, keepdims=True)
    sums = jnp.concatenate([gain_in, table_in], axis=1)
    everything = sent_to_all(sums, ("section", "dp")).reshape(sections, columns, -1)
    per_section = jnp.sum(everything, axis=1)
    gain_grad = lax.dynamic_index_in_dim(per_section, section_index, 0)[:, :shard_width]
    table_grad = jnp.sum(per_section[:, shard_width:], axis=0).reshape(shard_heads, bucket_count).T
    return (jnp.stack([first[:seq_len], second[:seq_len]])[None], gain_grad, table_grad)


def solution(mesh):
    in_specs = (
        P("dp", None, "mp"),
        P("dp", None, "mp"),
        P("dp", None),
        P(),
        P(None, "mp"),
        P("section", None),
        P("section", None, "mp"),
        P("section", None, "mp"),
        P("section", None, "mp"),
        P("section", None, "mp"),
    )
    out_specs = (P("section", "dp", None, "mp"), P("section", "mp"), P(None, "mp"))
    return jax.shard_map(
        per_device, mesh=mesh, in_specs=in_specs, out_specs=out_specs, check_vma=False
    )
```

```python
import functools

import jax
import jax.numpy as jnp
from jax import lax
from jax.experimental import pallas as pl
from jax.experimental.pallas import tpu as pltpu
from jax.sharding import PartitionSpec as P


neg_fill = -1000000000.0
epsilon = 1e-06
f32 = jnp.float32
bf16 = jnp.bfloat16
LANES = 128
EXTRA = 16
BY_ROWS = (((1,), (1,)), ((), ()))
BY_COLUMNS = (((0,), (0,)), ((), ()))
IN_VMEM = pl.BlockSpec(memory_space=pltpu.VMEM)
IN_SMEM = pl.BlockSpec(memory_space=pltpu.SMEM)


def sent_to_all(value, axis):
    devices = lax.axis_size(axis)
    return lax.all_to_all(
        jnp.broadcast_to(value[None], (devices, *value.shape)), axis, 0, 0, tiled=True
    )


def passed_along(block, axis, distance):
    devices = range(lax.axis_size(axis))
    route = [(i - distance, i) for i in devices if i - distance in devices]
    return lax.ppermute(block, axis, route)


def spread(index, planes):
    side = 4
    return (index % side) * (planes // side) + index // side


def plane_routes(sections, planes, columns, taking_part, back):
    routes = []
    for flip in (0, 1):
        route = []
        for s in taking_part:
            for m in range(planes):
                for d in range(columns):
                    sequence = 2 * d + (m % 2 ^ flip)
                    home = (s * planes + m) * columns + d
                    work = (s * planes + spread(sequence, planes)) * columns + m // 2
                    route.append((work, home) if back else (home, work))
        routes.append(route)
    return routes


def exchanged(pieces, sections, planes, columns, plane_index, taking_part, back=False):
    home_odd = plane_index % 2 == 1
    work_odd = spread(plane_index, planes) % 2 == 1
    sent_odd, came_odd = (work_odd, home_odd) if back else (home_odd, work_odd)
    arrived = []
    for flip, route in enumerate(plane_routes(sections, planes, columns, taking_part, back)):
        piece = jnp.where(sent_odd, pieces[1 - flip], pieces[flip])
        arrived.append(lax.ppermute(piece, ("section", "mp", "dp"), route))
    first, second = arrived
    return jnp.where(came_odd, second, first), jnp.where(came_odd, first, second)


def as_rows(column):
    rows = column.shape[0]
    high = column.astype(bf16).astype(f32)
    rest = column - high
    middle = rest.astype(bf16).astype(f32)
    low = rest - middle
    lane = lax.broadcasted_iota(jnp.int32, (rows, LANES), 1)
    spread = jnp.where(lane == 0, high, jnp.where(lane == 1, middle, jnp.where(lane == 2, low, 0.0)))
    square = jnp.concatenate([spread, jnp.zeros((LANES - rows, LANES), f32)], axis=0)
    return square.T[:EXTRA].astype(bf16)


def in_pieces(row):
    high = lax.reduce_precision(row, 8, 7)
    rest = row - high
    middle = lax.reduce_precision(rest, 8, 7)
    return jnp.concatenate([high, middle, rest - middle], axis=0).astype(bf16)


def as_column(extra, rows):
    total = jnp.sum(extra[:8], axis=0, keepdims=True)
    return jnp.broadcast_to(total, (LANES, LANES)).T[:rows]


def head_lanes(shape, which, head_dim):
    lane = lax.broadcasted_iota(jnp.int32, shape, 1)
    return (lane >= which * head_dim) & (lane < (which + 1) * head_dim)


def only_head(tile, which, head_dim):
    return jnp.where(head_lanes(tile.shape, which, head_dim), tile, jnp.zeros_like(tile))


def cut_kernel(column_ref, query_ref, key_ref, value_ref, out_ref, piece_ref, block_ref, sems):
    rows = piece_ref.shape[0]
    out_rows = block_ref.shape[0]
    column = column_ref[0]
    at = pl.ds(pl.multiple_of(column * rows, rows), rows)
    out_at = pl.ds(pl.multiple_of(column * out_rows, out_rows), out_rows)
    copies = [
        pltpu.make_async_copy(
            ref.at[0, at, :], piece_ref.at[:, i * LANES : (i + 1) * LANES], sems.at[i]
        )
        for i, ref in enumerate((query_ref, key_ref, value_ref))
    ]
    copies.append(pltpu.make_async_copy(out_ref.at[0, out_at, :], block_ref, sems.at[3]))
    for copy in copies:
        copy.start()
    for copy in copies:
        copy.wait()


def order_kernel(plane_ref, *refs):
    *blocks, out_ref = refs
    planes = len(blocks)
    for k, block in enumerate(blocks):
        out_ref[lax.rem(plane_ref[0] + planes - k, planes)] = block[...]


def project_kernel(h_ref, gain_ref, w_ref, out_ref):
    seq = h_ref.shape[0]
    rows = h_ref[...].astype(f32)
    scaled = (rows * gain_ref[...]).astype(bf16)
    extra = as_rows(jnp.sum(rows * rows, axis=1, keepdims=True))
    for shard in range(w_ref.shape[0]):
        part = jnp.dot(scaled, w_ref[shard], preferred_element_type=f32)
        for kind in range(3):
            at = (2 * kind + shard % 2) * seq
            out_ref[shard // 2, at : at + seq, :] = part[:, kind * LANES : (kind + 1) * LANES].astype(bf16)
    for column in range(out_ref.shape[0]):
        out_ref[column, 6 * seq :, :] = extra


def attend_kernel(tick, head_dim, model_width, last_section, *refs):
    last = tick == last_section
    if tick:
        section_ref, parts_ref, bias_ref, h_ref, w_ref, *old = refs[:10]
        refs = refs[10:]
    else:
        section_ref, parts_ref, bias_ref, h_ref, w_ref = refs[:5]
        refs = refs[5:]
    kept = refs[:5]
    h_keep, raw_keep, proj_keep, prob_keep, inv_keep = kept
    seq = h_ref.shape[0]
    total = parts_ref[0].astype(f32)
    for column in range(1, parts_ref.shape[0]):
        total = total + parts_ref[column].astype(f32)
    inv_rms = lax.rsqrt(as_column(total[6 * seq :], seq) / model_width + epsilon)
    raw = total[: 6 * seq]
    proj = (raw * jnp.concatenate([inv_rms] * 6, axis=0)).astype(bf16)
    tiles = [proj[i * seq : (i + 1) * seq] for i in range(6)]
    probs = []
    mixed = []
    for j in range(2):
        sum_tile = None
        for which in range(2):
            scores = lax.dot_general(
                only_head(tiles[j], which, head_dim), tiles[2 + j], BY_ROWS, preferred_element_type=f32
            )
            scores = scores + bias_ref[2 * j + which]
            exp_scores = jnp.exp(scores - jnp.max(scores, axis=-1, keepdims=True))
            prob = exp_scores / jnp.sum(exp_scores, axis=-1, keepdims=True)
            probs.append(prob)
            part = jnp.dot(
                prob.astype(bf16), only_head(tiles[4 + j], which, head_dim), preferred_element_type=f32
            )
            sum_tile = part if sum_tile is None else sum_tile + part
        mixed.append(sum_tile.astype(bf16))

    def store():
        h_keep[...] = h_ref[...]
        raw_keep[...] = raw
        proj_keep[...] = proj
        for i in range(4):
            prob_keep[i] = probs[i]
        inv_keep[...] = inv_rms

    if tick:
        mine = section_ref[0] == tick
        pl.when(mine)(store)

        @pl.when(jnp.logical_not(mine))
        def _():
            for new, before in zip(kept, old):
                new[...] = before[...]
    else:
        store()
    if not last:
        out_ref = refs[5]
        mixed_rows = jnp.concatenate(mixed, axis=1)

        def send():
            for shard in range(w_ref.shape[0]):
                at = 2 * (shard % 2) * LANES
                out_ref[shard // 2, :, at : at + 2 * LANES] = jnp.dot(
                    mixed_rows, w_ref[shard], preferred_element_type=f32
                ).astype(bf16)

        if tick:
            send()
        else:
            pl.when(section_ref[0] != last_section)(send)

            @pl.when(section_ref[0] == last_section)
            def _():
                for column in range(out_ref.shape[0]):
                    out_ref[column] = h_ref[...]


def attend_back_kernel(tick, section, head_dim, *refs):
    if tick:
        section_ref, up_ref, raw_ref, proj_ref, prob_ref, inv_ref, w_ref, old_ref, out_ref, score_ref = refs
    else:
        section_ref, up_ref, raw_ref, proj_ref, prob_ref, inv_ref, w_ref, out_ref, score_ref = refs
    seq = up_ref.shape[1]
    inner = 2 * LANES
    grad = jnp.zeros((seq, inner), f32)
    for shard in range(w_ref.shape[0]):
        at = 2 * (shard % 2) * LANES
        grad = grad + lax.dot_general(
            up_ref[shard // 2, :, at : at + inner],
            w_ref[shard],
            BY_ROWS,
            preferred_element_type=f32,
        )
    mixed_grad = grad.astype(bf16)
    tiles = [proj_ref[i * seq : (i + 1) * seq, :] for i in range(6)]
    grads = [None] * 6
    score_grads = []

    def add(i, value):
        grads[i] = value if grads[i] is None else grads[i] + value

    for j in range(2):
        grad_tile = mixed_grad[:, j * LANES : (j + 1) * LANES]
        for which in range(2):
            prob = prob_ref[2 * j + which]
            grad_head = only_head(grad_tile, which, head_dim)
            prob_grad = lax.dot_general(grad_head, tiles[4 + j], BY_ROWS, preferred_element_type=f32)
            add(4 + j, lax.dot_general(prob.astype(bf16), grad_head, BY_COLUMNS, preferred_element_type=f32))
            score_grad = prob * (prob_grad - jnp.sum(prob_grad * prob, axis=-1, keepdims=True))
            score_half = score_grad.astype(bf16)
            score_grads.append(score_grad)
            add(j, jnp.dot(score_half, only_head(tiles[2 + j], which, head_dim), preferred_element_type=f32))
            add(
                2 + j,
                lax.dot_general(
                    score_half, only_head(tiles[j], which, head_dim), BY_COLUMNS, preferred_element_type=f32
                ),
            )
    radial = None
    inv_rms = inv_ref[...]
    for i in range(6):
        part = grads[i] * raw_ref[i * seq : (i + 1) * seq, :]
        radial = part if radial is None else radial + part
        scaled = (grads[i] * inv_rms).astype(bf16)
        for column in range(out_ref.shape[0]):
            out_ref[column, i * seq : (i + 1) * seq, :] = scaled
    extra = as_rows(jnp.sum(radial, axis=1, keepdims=True))
    for column in range(out_ref.shape[0]):
        out_ref[column, 6 * seq :, :] = extra

    def store():
        for i in range(4):
            score_ref[i] = score_grads[i]

    if tick:
        mine = section_ref[0] == section
        pl.when(mine)(store)

        @pl.when(jnp.logical_not(mine))
        def _():
            score_ref[...] = old_ref[...]
    else:
        store()


def input_kernel(tick, section, last, model_width, *refs):
    section_ref, parts_ref, up_ref, h_ref, gain_ref, inv_ref, w_ref, *rest = refs
    grad_keep, gain_keep = rest[-2:]
    seq, width = up_ref.shape
    normed = jnp.zeros((seq, width), f32)
    for shard in range(w_ref.shape[0]):
        left = jnp.concatenate(
            [
                parts_ref[shard // 2, (2 * kind + shard % 2) * seq : (2 * kind + shard % 2 + 1) * seq, :]
                for kind in range(3)
            ],
            axis=1,
        )
        normed = normed + lax.dot_general(
            left, w_ref[shard], BY_ROWS, preferred_element_type=f32
        )
    extra = parts_ref[0, 6 * seq :, :].astype(f32)
    for column in range(1, parts_ref.shape[0]):
        extra = extra + parts_ref[column, 6 * seq :, :].astype(f32)
    inv_rms = inv_ref[...]
    radial = as_column(extra, seq) * (inv_rms * inv_rms * inv_rms) / model_width
    rows = h_ref[...].astype(f32)
    repeats = width // LANES
    input_grad = (
        up_ref[...].astype(f32)
        + normed * gain_ref[...]
        - jnp.concatenate([radial] * repeats, axis=1) * rows
    ).astype(bf16)
    if not last:
        rest[-3][...] = input_grad
    gain_part = jnp.sum(normed * rows, axis=0, keepdims=True)

    def store():
        grad_keep[...] = input_grad
        gain_keep[...] = gain_part

    if tick:
        mine = section_ref[0] == section
        pl.when(mine)(store)

        @pl.when(jnp.logical_not(mine))
        def _():
            grad_keep[...] = rest[0][...]
            gain_keep[...] = rest[1][...]
    else:
        store()


def shaped(shape, dtype):
    return jax.ShapeDtypeStruct(shape, dtype)


def called(kernel, out_shape, flops, *args):
    specs = [IN_SMEM if a.dtype == jnp.int32 else IN_VMEM for a in args]
    outs = jax.tree.map(lambda _: IN_VMEM, out_shape)
    return pl.pallas_call(
        kernel,
        out_shape=out_shape,
        in_specs=specs,
        out_specs=outs,
        cost_estimate=pl.CostEstimate(flops=flops, bytes_accessed=8 << 20, transcendentals=16384),
        compiler_params=pltpu.CompilerParams(vmem_limit_bytes=16 << 20),
    )(*args)


def per_device(
    stream, cotangent, token_ids, buckets, bias_table, gain, w_query, w_key, w_value, w_out
):
    sections = lax.axis_size("section")
    planes = lax.axis_size("mp")
    columns = lax.axis_size("dp")
    section_index = lax.axis_index("section")
    plane_index = lax.axis_index("mp")
    column_index = lax.axis_index("dp")
    section_at = section_index.astype(jnp.int32).reshape(1)
    bucket_count, shard_heads = bias_table.shape
    table_size = bucket_count * shard_heads
    seq_len, shard_width = stream.shape[1:]
    model_width = gain.shape[1]
    width = model_width // columns
    head_dim = w_query.shape[2] // shard_heads
    heads_local = 2 * shard_heads

    in_hbm = pl.BlockSpec(memory_space=pl.ANY)
    out_rows = w_out.shape[1] // columns
    piece, block = pl.pallas_call(
        cut_kernel,
        out_shape=[shaped((width, 3 * LANES), bf16), shaped((out_rows, shard_width), bf16)],
        in_specs=[IN_SMEM] + [in_hbm] * 4,
        out_specs=[IN_VMEM, IN_VMEM],
        scratch_shapes=[pltpu.SemaphoreType.DMA((4,))],
    )(column_index.astype(jnp.int32).reshape(1), w_query, w_key, w_value, w_out)
    weights = lax.all_gather(piece, "mp", axis=0, tiled=True).reshape(planes, *piece.shape)
    up, down = [block], [block]
    for _ in range(planes // 2):
        up.append(lax.ppermute(up[-1], "mp", [(i, (i + 1) % planes) for i in range(planes)]))
    for _ in range(planes // 2 - 1):
        down.append(lax.ppermute(down[-1], "mp", [(i, (i - 1) % planes) for i in range(planes)]))
    plane_at = plane_index.astype(jnp.int32).reshape(1)

    def planed(pieces, taking_part=range(sections), back=False):
        return exchanged(pieces, sections, planes, columns, plane_index, taking_part, back)

    is_last = section_index == sections - 1
    own = [jnp.where(is_last, cotangent[i], stream[i]) for i in (0, 1)]
    entering = jnp.concatenate(planed(own, (0, sections - 1)), axis=1)
    masks = jnp.where(token_ids == 0, neg_fill, 0.0).astype(f32)
    flat_bias = bias_table.reshape(1, -1)
    low, high = planed([jnp.concatenate([flat_bias, masks[i : i + 1]], axis=1) for i in (0, 1)])
    mask_row = low[0, flat_bias.shape[1] :]
    bias_local = jnp.concatenate(
        [p[0, : flat_bias.shape[1]].reshape(bucket_count, shard_heads) for p in (low, high)], axis=1
    )
    gain_share = lax.dynamic_slice_in_dim(gain, column_index * width, width, axis=1)
    onehot = (
        buckets[:, :, None] == jnp.arange(bucket_count, dtype=jnp.int32)[None, None, :]
    ).astype(f32)
    bias_heads = jnp.einsum("qkb,bh->hqk", onehot, bias_local, precision=lax.Precision.HIGHEST)
    score_bias = bias_heads + mask_row[None, None, :]
    out_weights = called(
        order_kernel, shaped((planes, *block.shape), bf16), 1, plane_at, *up, *down[:0:-1]
    )
    entering, score_bias, section_at, gain_share, out_weights = lax.optimization_barrier(
        (entering, score_bias, section_at, gain_share, out_weights)
    )

    tall = 6 * seq_len
    message = shaped((columns, tall + EXTRA, LANES), bf16)
    kept_shapes = [
        shaped((seq_len, width), bf16),
        shaped((tall, LANES), f32),
        shaped((tall, LANES), bf16),
        shaped((heads_local, seq_len, seq_len), f32),
        shaped((seq_len, LANES), f32),
    ]
    project_flops = 6 * seq_len * model_width * LANES * planes
    out_flops = 2 * seq_len * 2 * LANES * model_width

    rows = entering
    kept = []
    for tick in range(sections):
        last = tick == sections - 1
        sent = called(project_kernel, message, project_flops, rows, gain_share, weights)
        parts = lax.all_to_all(sent, "dp", 0, 0, tiled=True)
        outs = list(kept_shapes)
        if not last:
            outs.append(shaped((columns, seq_len, width), bf16))
        kernel = functools.partial(attend_kernel, tick, head_dim, model_width, sections - 1)
        done = called(kernel, outs, out_flops, section_at, parts, score_bias, rows, out_weights, *kept)
        kept = list(done[:5])
        if not last:
            branch = lax.all_to_all(done[5], "dp", 0, 0, tiled=True)
            if tick == 0:
                up_all = branch
            rows = (rows.astype(f32) + jnp.sum(branch.astype(f32), axis=0)).astype(bf16)
            rows = passed_along(rows, "section", 1)
    h_rows, raw, proj, probs, inv_rms = kept

    upstream = entering
    scores = []
    grads = []
    for tick in range(sections):
        section = sections - 1 - tick
        if tick:
            up_all = sent_to_all(upstream, "dp")
        kernel = functools.partial(attend_back_kernel, tick, section, head_dim)
        outs = [message, shaped((heads_local, seq_len, seq_len), f32)]
        sent, score_grad = called(
            kernel, outs, out_flops, section_at, up_all, raw, proj, probs, inv_rms, out_weights, *scores
        )
        scores = [score_grad]
        last = tick == sections - 1
        parts = lax.all_to_all(sent, "dp", 0, 0, tiled=True)
        kernel = functools.partial(input_kernel, tick, section, last, model_width)
        share = shaped((seq_len, width), bf16)
        keep = [share, shaped((1, width), f32)]
        outs = keep if last else [share, *keep]
        done = called(
            kernel,
            outs,
            project_flops,
            section_at,
            parts,
            upstream,
            h_rows,
            gain_share,
            inv_rms,
            weights,
            *grads,
        )
        grads = list(done[-2:])
        if not last:
            upstream = passed_along(done[0], "section", -1)

    score_grad, gain_part = lax.optimization_barrier((scores[0], grads[1]))
    table_part = jnp.einsum("qkb,hqk->hb", onehot, score_grad, precision=lax.Precision.HIGHEST)
    table_row = jnp.pad(table_part.reshape(2, -1), ((0, 0), (0, shard_width - table_size)))
    riding = jnp.concatenate(
        [
            in_pieces(gain_part),
            in_pieces(table_row.reshape(1, -1)),
            jnp.zeros((EXTRA - 6, width), bf16),
        ],
        axis=0,
    )
    going = jnp.concatenate([grads[0], riding], axis=0)
    first, second = planed([going[:, :shard_width], going[:, shard_width:]], back=True)
    rows_in = first[seq_len:].astype(f32) + second[seq_len:].astype(f32)
    gain_in = jnp.sum(rows_in[:3], axis=0, keepdims=True)
    table_in = jnp.sum(rows_in[3:6, :table_size], axis=0, keepdims=True)
    sums = jnp.concatenate([gain_in, table_in], axis=1)
    everything = sent_to_all(sums, ("section", "dp")).reshape(sections, columns, -1)
    per_section = jnp.sum(everything, axis=1)
    gain_grad = lax.dynamic_index_in_dim(per_section, section_index, 0)[:, :shard_width]
    table_grad = jnp.sum(per_section[:, shard_width:], axis=0).reshape(shard_heads, bucket_count).T
    return (jnp.stack([first[:seq_len], second[:seq_len]])[None], gain_grad, table_grad)


def solution(mesh):
    in_specs = (
        P("dp", None, "mp"),
        P("dp", None, "mp"),
        P("dp", None),
        P(),
        P(None, "mp"),
        P("section", None),
        P("section", None, "mp"),
        P("section", None, "mp"),
        P("section", None, "mp"),
        P("section", None, "mp"),
    )
    out_specs = (P("section", "dp", None, "mp"), P("section", "mp"), P(None, "mp"))
    return jax.shard_map(
        per_device, mesh=mesh, in_specs=in_specs, out_specs=out_specs, check_vma=False
    )
```
